256 devices in a mesh: dp: 8 (over x_lo, y), mp: 32 (over z, x_hi, core).
Axes of the slice: x: 4 (x_hi: 2, x_lo: 2; x = x_hi * 2 + x_lo), y: 4, z: 8, core: 2. Of those that a mesh axis runs over, the one named last changes fastest.
Arguments:
- tokens: bfloat16 [1024, 6144], P(('dp', 'mp')), may hold values from -6 to 6
- norm_gain: float32 [6144], replicated, may hold values from 0.5 to 1.5
- w_query: bfloat16 [6144, 4096], P('dp', 'mp'), as said below
- w_key: bfloat16 [6144, 4096], P('dp', 'mp'), as said below
- w_value: bfloat16 [6144, 4096], P('dp', 'mp'), may hold values from -0.078125 to 0.078125
- w_inner: bfloat16 [6144, 24576], P('dp', 'mp'), may hold values from -0.078125 to 0.078125
- bias_inner: float32 [24576], P('mp'), may hold values from -3 to 3
- w_attn_out: bfloat16 [4096, 6144], P('mp', 'dp'), may hold values from -0.09375 to 0.09375
- w_outer: bfloat16 [24576, 6144], P('mp', 'dp'), may hold values from -0.0390625 to 0.0390625
- temper: float32 [32], P('mp'), may hold values from 0.5 to 24
Outputs:
- result: bfloat16 [1024, 6144], P(('dp', 'mp'))
The draws below stay inside these ranges and needn't reach their ends.
Inputs may be any that keep to these rules, and one draw needn't show every extreme that they name: `w_query`: entries of order 6144 ** -0.5. `w_key`: entries of order 6144 ** -0.5.
All inputs are finite; a program needn't handle non-finite values.
Results may differ from the reference program's by a relative error of at most 0.023.
Values may be sent and summed in bfloat16 or wider, within the bound.
No kernel may reach another device: no remote copies, remote signals or barrier semaphores. Data moves between devices by JAX's collectives and lax.ppermute only.
A program may use at most 64 MiB of HBM per device.

```python
import math
import jax
import jax.numpy as jnp
from jax import lax

D = 6144
HEADS = 32
HEAD = 128
FF = 24576
HD = 4096
PATCHES = 128
TOKENS = 1024
N_DP = 8


def shared_draws(key):
    key_query = jax.random.fold_in(key, 11)
    key_noise = jax.random.fold_in(key, 12)
    key_temper = jax.random.fold_in(key, 14)
    scale = D ** (-0.5)
    limit = 6.0 * scale
    query = jnp.clip(jax.random.normal(key_query, (D, HD), jnp.float32) * scale, -limit, limit)
    noise = jnp.clip(jax.random.normal(key_noise, (D, HD), jnp.float32) * scale, -limit, limit)
    temper = jnp.exp(jax.random.uniform(key_temper, (HEADS,), jnp.float32, jnp.log(0.5), jnp.log(6.0)))
    keys = noise
    return (query, keys, temper)


def draw_w_query(key, part):
    return shared_draws(key)[0].astype(jnp.bfloat16)


def draw_w_key(key, part):
    return shared_draws(key)[1].astype(jnp.bfloat16)


def draw_temper(key, part):
    return shared_draws(key)[2]


def level_of(rng, extent, split, low, high):
    level, own = 1.0, jax.random.fold_in(rng, 6)
    for dim, blocks in split:
        heights = jnp.exp(jax.random.uniform(jax.random.fold_in(own, dim), (blocks,), jnp.float32, low / len(split), high / len(split)))
        level = level * jnp.repeat(heights, extent[dim] // blocks).reshape([-1 if axis == dim else 1 for axis in range(len(extent))])
    return level


def bell_draw(stream_key, extent, deviation, most, shards=(), kind=jnp.bfloat16):
    result = deviation * jax.random.normal(stream_key, extent, jnp.float32)
    if shards:
        result = result * level_of(stream_key, extent, shards, -0.22, 0.18)
    return jnp.clip(result, -most, most).astype(kind)


def setup_inputs(seed: int = 0) -> dict:
    streams_of = jax.random.split(jax.random.key(seed), 11)
    return {
        "tokens": bell_draw(streams_of[0], (TOKENS, D), 1.0, 6.0, ((0, 256),)),
        "norm_gain": jnp.clip(1.0 + 0.1 * jax.random.normal(streams_of[1], (D,), jnp.float32), 0.5, 1.5),
        "w_query": draw_w_query(jax.random.fold_in(streams_of[10], 71), 0),
        "w_key": draw_w_key(jax.random.fold_in(streams_of[10], 71), 0),
        "w_value": bell_draw(streams_of[4], (D, HD), D ** -0.5, 0.078125, ((0, 8), (1, 32))),
        "w_inner": bell_draw(streams_of[5], (D, FF), D ** -0.5, 0.078125, ((0, 8), (1, 32))),
        "bias_inner": bell_draw(streams_of[6], (FF,), 0.5, 3.0, ((0, 32),), jnp.float32),
        "w_attn_out": bell_draw(streams_of[7], (HD, D), HD ** -0.5, 0.09375, ((0, 32), (1, 8))),
        "w_outer": bell_draw(streams_of[8], (FF, D), FF ** -0.5, 0.0390625, ((0, 32), (1, 8))),
        "temper": draw_temper(jax.random.fold_in(streams_of[10], 71), 0),
    }


def normalize(values):
    center = values - lax.optimization_barrier(jnp.mean(values, axis=-1, keepdims=True))
    spread = lax.optimization_barrier(jnp.mean(center * center, axis=-1, keepdims=True))
    return center * lax.rsqrt(spread + 1e-06)

def reference(tokens, norm_gain, w_query, w_key, w_value, w_inner, bias_inner, w_attn_out, w_outer, temper):
    local = tokens.astype(jnp.float32)
    normed = (normalize(local) * norm_gain.astype(jnp.float32)).astype(jnp.bfloat16)
    query = jnp.dot(normed, w_query, preferred_element_type=jnp.float32).astype(jnp.bfloat16)
    keys = jnp.dot(normed, w_key, preferred_element_type=jnp.float32).astype(jnp.bfloat16)
    values = jnp.dot(normed, w_value, preferred_element_type=jnp.float32).astype(jnp.bfloat16)
    shape = (N_DP, PATCHES, HEADS, HEAD)
    query_norm = normalize(query.astype(jnp.float32).reshape(shape)).astype(jnp.bfloat16)
    key_norm = normalize(keys.astype(jnp.float32).reshape(shape)).astype(jnp.bfloat16)
    values4 = values.reshape(shape).astype(jnp.float32)
    scale = temper.astype(jnp.float32) / math.sqrt(HEAD)
    scores = jnp.einsum('bqhc,bkhc->bhqk', query_norm.astype(jnp.float32), key_norm.astype(jnp.float32))
    scores = scores * scale[None, :, None, None]
    probs = jax.nn.softmax(scores, axis=-1).astype(jnp.bfloat16)
    mixed = jnp.einsum('bhqk,bkhc->bqhc', probs.astype(jnp.float32), values4)
    mixed = mixed.astype(jnp.bfloat16).reshape(TOKENS, HD)
    inner = jnp.dot(normed, w_inner, preferred_element_type=jnp.float32) + bias_inner.astype(jnp.float32)
    activ = jax.nn.gelu(inner, approximate=False).astype(jnp.bfloat16)
    total = jnp.dot(mixed, w_attn_out, preferred_element_type=jnp.float32)
    total = total + jnp.dot(activ, w_outer, preferred_element_type=jnp.float32)
    return (local + total).astype(jnp.bfloat16)
```

```python
import math

import jax
import jax.numpy as jnp
from jax import lax
from jax.sharding import Mesh
from jax.sharding import PartitionSpec as P

HEAD = 128
DP = ("xl", "y")
MP = ("z", "xh", "c")
ALL = DP + MP
BF = jnp.bfloat16
F32 = jnp.float32


def normalize(values):
    center = values - jnp.mean(values, axis=-1, keepdims=True)
    spread = jnp.mean(center * center, axis=-1, keepdims=True)
    return center * lax.rsqrt(spread + 1e-06)


def partner(array, axis):
    return lax.ppermute(array, axis, [(0, 1), (1, 0)])


def exchange(pieces, axes):
    return lax.all_to_all(pieces, axes, split_axis=0, concat_axis=0, tiled=True)


def dot(a, b):
    return lax.dot_general(a, b, (((a.ndim - 1,), (0,)), ((), ())), preferred_element_type=F32)


def own_first(array, dim):
    flipped = jnp.flip(array, dim)
    return jnp.where(lax.axis_index("xl") == 0, array, flipped)


def per_device(
    tokens, norm_gain, w_query, w_key, w_value, w_inner, bias_inner, w_attn_out, w_outer, temper
):
    count, width = tokens.shape
    n_xl, n_y, n_z, n_xh = (lax.axis_size(a) for a in ("xl", "y", "z", "xh"))
    block = width // (n_xl * n_y)
    local = tokens.astype(F32)
    normed = (normalize(local) * norm_gain).astype(BF)
    beside = partner(normed, "xh")
    first = lax.axis_index("xh") == 0
    rows = jnp.concatenate(
        (jnp.where(first, normed, beside), jnp.where(first, beside, normed)), axis=0
    )
    w_qkv = jnp.concatenate((w_query, w_key, w_value), axis=1)
    w_out = jnp.concatenate((w_attn_out, w_outer), axis=0)
    rows, w_qkv_s, w_inner_s, w_out_s = lax.optimization_barrier((rows, w_qkv, w_inner, w_out))
    w_qkv_p = partner(w_qkv_s, "xl")
    w_inner_p = partner(w_inner_s, "xl")
    w_out_p = partner(w_out_s, "xl")
    split = own_first(rows.reshape(n_xh * count, n_xl, n_y, block), 1)
    split = split.transpose(2, 0, 1, 3)
    pieces = jnp.broadcast_to(
        split[:, None], (n_y, n_z, n_xh * count, n_xl, block)
    ).reshape(n_y * n_z, n_xh * count, n_xl * block)
    mine = exchange(pieces, ("y", "z")).reshape(n_y, -1, n_xl * block)
    theirs = partner(mine, "c")
    image = jnp.concatenate((mine, theirs), axis=1)
    patches = image.shape[1]

    def projected(weights, weights_p):
        partial = dot(image[..., :block], weights) + dot(image[..., block:], weights_p)
        arrived = exchange(partial.astype(BF), "y")
        return arrived.astype(F32).sum(axis=0)

    qkv = projected(w_qkv, w_qkv_p)
    query_norm = normalize(qkv[:, :HEAD].astype(BF).astype(F32)).astype(BF)
    key_norm = normalize(qkv[:, HEAD : 2 * HEAD].astype(BF).astype(F32)).astype(BF)
    value = qkv[:, 2 * HEAD :].astype(BF)
    scores = jnp.einsum("qc,kc->qk", query_norm, key_norm, preferred_element_type=F32)
    scores = scores * (temper / math.sqrt(HEAD))
    probs = jax.nn.softmax(scores, axis=-1).astype(BF)
    mixed = dot(probs, value).astype(BF)
    inner = projected(w_inner, w_inner_p) + bias_inner
    activ = jax.nn.gelu(inner, approximate=False).astype(BF)
    features = jnp.concatenate((mixed, activ), axis=1)
    features = exchange(jnp.broadcast_to(features, (n_y, *features.shape)), "y")
    half = patches // 2

    def output(part):
        return jnp.concatenate((dot(part, w_out), dot(part, w_out_p)), axis=-1)

    sent = output(features[:, half:]).astype(BF)
    summed = (output(features[:, :half]) + partner(sent, "c").astype(F32)).astype(BF)
    pieces = summed.reshape(n_y * n_z * n_xh, count, n_xl * block)
    arrived = exchange(pieces, ("y", "z", "xh"))
    total = arrived.reshape(n_y, n_z * n_xh, count, n_xl, block).astype(F32).sum(axis=1)
    total = own_first(total.transpose(1, 2, 0, 3), 1).reshape(count, width)
    return (local + total).astype(BF)


def solution(mesh):
    finer = Mesh(mesh.devices.reshape(2, 4, 8, 2, 2), ALL)
    return jax.shard_map(
        per_device,
        mesh=finer,
        in_specs=(
            P(ALL, None),
            P(),
            P(DP, MP),
            P(DP, MP),
            P(DP, MP),
            P(DP, MP),
            P(MP),
            P(MP, DP),
            P(MP, DP),
            P(MP),
        ),
        out_specs=P(ALL, None),
        check_vma=False,
    )
```

```python
import math

import jax
import jax.numpy as jnp
from jax import lax
from jax.sharding import Mesh
from jax.sharding import PartitionSpec as P


HEAD = 128
DP = ("xl", "y")
MP = ("z", "xh", "c")
ALL = DP + MP
BF = jnp.bfloat16
F32 = jnp.float32


def normalize(values):
    center = values - jnp.mean(values, axis=-1, keepdims=True)
    spread = jnp.mean(center * center, axis=-1, keepdims=True)
    return center * lax.rsqrt(spread + 1e-06)


def partner(array, axis):
    return lax.ppermute(array, axis, [(0, 1), (1, 0)])


def exchange(pieces, axes):
    return lax.all_to_all(pieces, axes, split_axis=0, concat_axis=0, tiled=True)


def dot(a, b):
    return lax.dot_general(a, b, (((a.ndim - 1,), (0,)), ((), ())), preferred_element_type=F32)


def own_first(array, dim):
    flipped = jnp.flip(array, dim)
    return jnp.where(lax.axis_index("xl") == 0, array, flipped)


def block(
    tokens, norm_gain, w_query, w_key, w_value, w_inner, bias_inner, w_attn_out, w_outer, temper
):
    count, width = tokens.shape
    n_xl, n_y, n_z, n_xh = (lax.axis_size(a) for a in ("xl", "y", "z", "xh"))
    cols = width // (n_xl * n_y)
    local = tokens.astype(F32)
    normed = (normalize(local) * norm_gain).astype(BF)
    beside = partner(normed, "xh")
    first = lax.axis_index("xh") == 0
    rows = jnp.concatenate(
        (jnp.where(first, normed, beside), jnp.where(first, beside, normed)), axis=0
    )
    w_qkv = jnp.concatenate((w_query, w_key, w_value), axis=1)
    w_out = jnp.concatenate((w_attn_out, w_outer), axis=0)
    w_qkv_p = partner(w_qkv, "xl")
    w_inner_p = partner(w_inner, "xl")
    w_out_p = partner(w_out, "xl")
    split = own_first(rows.reshape(n_xh * count, n_xl, n_y, cols), 1)
    split = split.transpose(2, 0, 1, 3)
    pieces = jnp.broadcast_to(
        split[:, None], (n_y, n_z, n_xh * count, n_xl, cols)
    ).reshape(n_y * n_z, n_xh * count, n_xl * cols)
    mine = exchange(pieces, ("y", "z"))
    mine = mine.reshape(n_y, -1, n_xl * cols)
    theirs = partner(mine, "c")
    image = jnp.concatenate((mine, theirs), axis=1)
    patches = image.shape[1]

    def projected(weights, weights_p):
        partial = dot(image[..., :cols], weights) + dot(image[..., cols:], weights_p)
        arrived = exchange(partial.astype(BF), "y")
        return arrived.astype(F32).sum(axis=0)

    qkv = projected(w_qkv, w_qkv_p)
    query_norm = normalize(qkv[:, :HEAD].astype(BF).astype(F32)).astype(BF)
    key_norm = normalize(qkv[:, HEAD : 2 * HEAD].astype(BF).astype(F32)).astype(BF)
    value = qkv[:, 2 * HEAD :].astype(BF)
    scores = jnp.einsum("qc,kc->qk", query_norm, key_norm, preferred_element_type=F32)
    scores = scores * (temper / math.sqrt(HEAD))
    probs = jax.nn.softmax(scores, axis=-1).astype(BF)
    mixed = dot(probs, value).astype(BF)
    inner = projected(w_inner, w_inner_p) + bias_inner
    activ = jax.nn.gelu(inner, approximate=False).astype(BF)
    features = jnp.concatenate((mixed, activ), axis=1)
    features = exchange(jnp.broadcast_to(features, (n_y, *features.shape)), "y")
    half = patches // 2

    def output(part):
        return jnp.concatenate((dot(part, w_out), dot(part, w_out_p)), axis=-1)

    sent = output(features[:, half:]).astype(BF)
    summed = (output(features[:, :half]) + partner(sent, "c").astype(F32)).astype(BF)
    pieces = summed.reshape(n_y * n_z * n_xh, count, n_xl * cols)
    arrived = exchange(pieces, ("y", "z", "xh"))
    total = arrived.reshape(n_y, n_z * n_xh, count, n_xl, cols).astype(F32).sum(axis=1)
    total = own_first(total.transpose(1, 2, 0, 3), 1).reshape(count, width)
    return (local + total).astype(BF)


def solution(mesh):
    finer = Mesh(mesh.devices.reshape(2, 4, 8, 2, 2), ALL)
    return jax.shard_map(
        block,
        mesh=finer,
        in_specs=(
            P(ALL, None),
            P(),
            P(DP, MP),
            P(DP, MP),
            P(DP, MP),
            P(DP, MP),
            P(MP),
            P(MP, DP),
            P(MP, DP),
            P(MP),
        ),
        out_specs=P(ALL, None),
        check_vma=False,
    )
```

```python
import math

import jax
import jax.numpy as jnp
from jax import lax
from jax.experimental import pallas as pl
from jax.experimental.pallas import tpu as pltpu
from jax.sharding import Mesh
from jax.sharding import PartitionSpec as P


HEAD = 128
DP = ("xl", "y")
MP = ("z", "xh", "c")
ALL = DP + MP
BF = jnp.bfloat16
F32 = jnp.float32


def normalize(values):
    center = values - jnp.mean(values, axis=-1, keepdims=True)
    spread = jnp.mean(center * center, axis=-1, keepdims=True)
    return center * lax.rsqrt(spread + 1e-06)


def partner(array, axis):
    return lax.ppermute(array, axis, [(0, 1), (1, 0)])


def exchange(pieces, axes):
    return lax.all_to_all(pieces, axes, split_axis=0, concat_axis=0, tiled=True)


def dot(a, b):
    return lax.dot_general(a, b, (((a.ndim - 1,), (0,)), ((), ())), preferred_element_type=F32)


def own_first(array, dim):
    flipped = jnp.flip(array, dim)
    return jnp.where(lax.axis_index("xl") == 0, array, flipped)


def project_kernel(mine, theirs, *refs):
    sources = refs[:4]
    out = refs[4]
    tokens, kept, sems = refs[5:7], refs[7:11], refs[11]
    copies = [
        pltpu.make_async_copy(src, dst, sems.at[n])
        for n, (src, dst) in enumerate(zip((mine, theirs, *sources), (*tokens, *kept)))
    ]
    for copy in (copies[0], copies[2], copies[3], copies[1], copies[4], copies[5]):
        copy.start()
    images, half, width = tokens[0].shape
    cols = width // 2
    for n in (0, 2, 3):
        copies[n].wait()
    for part in range(2):
        if part:
            copies[1].wait()
        rows = tokens[part][...].reshape(images * half, width)
        for n in range(3):
            if not part and n == 1:
                for m in (4, 5):
                    copies[m].wait()
            w, w_p = kept[:2] if n == 0 else kept[2:]
            at = slice(0, 384) if n == 0 else slice((n - 1) * 384, n * 384)
            value = dot(rows[:, :cols], w[:, at]) + dot(rows[:, cols:], w_p[:, at])
            out[:, part * half : (part + 1) * half, n * 384 : (n + 1) * 384] = value.astype(
                BF
            ).reshape(images, half, 384)


def project(mine, theirs, *weights):
    images, half, width = mine.shape
    columns = weights[0].shape[1] + weights[2].shape[1]
    spec = pl.BlockSpec(memory_space=pl.ANY)
    return pl.pallas_call(
        project_kernel,
        out_shape=jax.ShapeDtypeStruct((images, 2 * half, columns), BF),
        in_specs=[spec] * 6,
        out_specs=pl.BlockSpec(memory_space=pltpu.VMEM),
        scratch_shapes=[pltpu.VMEM(mine.shape, BF)] * 2
        + [pltpu.VMEM(w.shape, BF) for w in weights]
        + [pltpu.SemaphoreType.DMA((6,))],
        compiler_params=pltpu.CompilerParams(vmem_limit_bytes=24 * 1024 * 1024),
        cost_estimate=pl.CostEstimate(
            flops=4 * images * half * width * columns,
            bytes_accessed=7 * 1024 * 1024,
            transcendentals=0,
        ),
        name="project",
    )(mine, theirs, *weights)


def block(
    tokens, norm_gain, w_query, w_key, w_value, w_inner, bias_inner, w_attn_out, w_outer, temper
):
    count, width = tokens.shape
    n_xl, n_y, n_z, n_xh = (lax.axis_size(a) for a in ("xl", "y", "z", "xh"))
    cols = width // (n_xl * n_y)
    local = tokens.astype(F32)
    normed = (normalize(local) * norm_gain).astype(BF)
    beside = partner(normed, "xh")
    first = lax.axis_index("xh") == 0
    rows = jnp.concatenate(
        (jnp.where(first, normed, beside), jnp.where(first, beside, normed)), axis=0
    )
    w_qkv = jnp.concatenate((w_query, w_key, w_value), axis=1)
    w_out = jnp.concatenate((w_attn_out, w_outer), axis=0)
    w_qkv_p = partner(w_qkv, "xl")
    w_inner_p = partner(w_inner, "xl")
    w_out_p = partner(w_out, "xl")
    split = own_first(rows.reshape(n_xh * count, n_xl, n_y, cols), 1)
    split = split.transpose(2, 0, 1, 3)
    pieces = jnp.broadcast_to(
        split[:, None], (n_y, n_z, n_xh * count, n_xl, cols)
    ).reshape(n_y * n_z, n_xh * count, n_xl * cols)
    mine = exchange(pieces, ("y", "z"))
    mine = mine.reshape(n_y, -1, n_xl * cols)
    theirs = partner(mine, "c")
    patches = 2 * mine.shape[1]
    partial = project(mine, theirs, w_qkv, w_qkv_p, w_inner, w_inner_p)
    sums = exchange(partial, "y").astype(F32).sum(axis=0)
    scale = temper / math.sqrt(HEAD)
    query_norm = normalize(sums[:, :HEAD].astype(BF).astype(F32)).astype(BF)
    key_norm = normalize(sums[:, HEAD : 2 * HEAD].astype(BF).astype(F32)).astype(BF)
    value = sums[:, 2 * HEAD : 3 * HEAD].astype(BF)
    scores = jnp.einsum("qc,kc->qk", query_norm, key_norm, preferred_element_type=F32)
    scores = scores * scale
    probs = jax.nn.softmax(scores, axis=-1).astype(BF)
    mixed = dot(probs, value).astype(BF)
    inner = sums[:, 3 * HEAD :] + bias_inner
    activ = jax.nn.gelu(inner, approximate=False).astype(BF)
    features = jnp.concatenate((mixed, activ), axis=1)
    features = exchange(jnp.broadcast_to(features, (n_y, *features.shape)), "y")
    half = patches // 2

    def output(part):
        return jnp.concatenate((dot(part, w_out), dot(part, w_out_p)), axis=-1)

    sent = output(features[:, half:]).astype(BF)
    summed = (output(features[:, :half]) + partner(sent, "c").astype(F32)).astype(BF)
    pieces = summed.reshape(n_y * n_z * n_xh, count, n_xl * cols)
    arrived = exchange(pieces, ("y", "z", "xh"))
    total = arrived.reshape(n_y, n_z * n_xh, count, n_xl, cols).astype(F32).sum(axis=1)
    total = own_first(total.transpose(1, 2, 0, 3), 1).reshape(count, width)
    return (local + total).astype(BF)


def solution(mesh):
    finer = Mesh(mesh.devices.reshape(2, 4, 8, 2, 2), ALL)
    return jax.shard_map(
        block,
        mesh=finer,
        in_specs=(
            P(ALL, None),
            P(),
            P(DP, MP),
            P(DP, MP),
            P(DP, MP),
            P(DP, MP),
            P(MP),
            P(MP, DP),
            P(MP, DP),
            P(MP),
        ),
        out_specs=P(ALL, None),
        check_vma=False,
    )
```

```python
import functools
import math

import jax
import jax.numpy as jnp
from jax import lax
from jax.experimental import pallas as pl
from jax.experimental.pallas import tpu as pltpu
from jax.sharding import Mesh
from jax.sharding import PartitionSpec as P


HEAD = 128
DP = ("xl", "y")
MP = ("z", "xh", "c")
ALL = DP + MP
BF = jnp.bfloat16
F32 = jnp.float32
ANY = pl.BlockSpec(memory_space=pl.ANY)
VMEM = pl.BlockSpec(memory_space=pltpu.VMEM)


def normalize(values):
    center = values - jnp.mean(values, axis=-1, keepdims=True)
    spread = jnp.mean(center * center, axis=-1, keepdims=True)
    return center * lax.rsqrt(spread + 1e-06)


def partner(array, axis):
    return lax.ppermute(array, axis, [(0, 1), (1, 0)])


def exchange(pieces, axes):
    return lax.all_to_all(pieces, axes, split_axis=0, concat_axis=0, tiled=True)


def dot(a, b):
    return lax.dot_general(a, b, (((a.ndim - 1,), (0,)), ((), ())), preferred_element_type=F32)


def params(mib):
    return pltpu.CompilerParams(vmem_limit_bytes=mib * 1024 * 1024)


def cost(flops, moved):
    return pl.CostEstimate(flops=flops, bytes_accessed=moved, transcendentals=0)


def spread_kernel(n_y, n_z, own, beside, gain, out):
    _, width = own.shape
    cols = width // (2 * n_y)
    mine, theirs = own[...].astype(F32), beside[...].astype(F32)
    first = lax.axis_index("xh") == 0
    rows = jnp.concatenate(
        (jnp.where(first, mine, theirs), jnp.where(first, theirs, mine)), axis=0
    )
    normed = normalize(rows) * gain[...]
    lower = lax.axis_index("xl") == 0
    for y in range(n_y):
        a = normed[:, y * cols : (y + 1) * cols]
        b = normed[:, (n_y + y) * cols : (n_y + y + 1) * cols]
        left = jnp.where(lower, a, b).astype(BF)
        right = jnp.where(lower, b, a).astype(BF)
        for z in range(n_z):
            out[y * n_z + z, :, :cols] = left
            out[y * n_z + z, :, cols:] = right


def spread(tokens, beside, gain, n_y, n_z):
    count, width = tokens.shape
    return pl.pallas_call(
        functools.partial(spread_kernel, n_y, n_z),
        out_shape=jax.ShapeDtypeStruct((n_y * n_z, 2 * count, width // n_y), BF),
        in_specs=[VMEM] * 3,
        out_specs=VMEM,
        compiler_params=params(8),
        cost_estimate=cost(20 * count * width, 2 * 1024 * 1024),
        name="normed_pieces",
    )(tokens, beside, gain.reshape(1, width))


def project_kernel(before, chunk, *refs):
    count = 4 + before
    sources, out = refs[:count], refs[count]
    kept, sems = refs[count + 1 : count + 5], refs[count + 5]
    done = []
    if before:
        width = sources[4].shape[-1]
        done = [
            pltpu.make_async_copy(
                sources[4], out.at[:, :, out.shape[-1] - width :], sems.at[4]
            )
        ]
    copies = [pltpu.make_async_copy(sources[n], kept[n], sems.at[n]) for n in range(4)]
    for n in (0, 2, 3, 1):
        copies[n].start()
    for copy in done:
        copy.start()
    images, half, width = kept[0].shape
    cols = width // 2
    for n in (0, 2, 3):
        copies[n].wait()
    w, w_p = kept[2], kept[3]
    for part in range(2):
        if part:
            copies[1].wait()
        rows = kept[part][...].reshape(images * half, width)
        for n in range(w.shape[1] // chunk):
            at = slice(n * chunk, (n + 1) * chunk)
            value = dot(rows[:, :cols], w[:, at]) + dot(rows[:, cols:], w_p[:, at])
            out[:, part * half : (part + 1) * half, at] = value.astype(BF).reshape(
                images, half, chunk
            )
    for copy in done:
        copy.wait()


def project(mine, theirs, weights, weights_p, before=None):
    images, half, width = mine.shape
    columns = weights.shape[1] + (0 if before is None else before.shape[-1])
    arrays = (mine, theirs, weights, weights_p) + (() if before is None else (before,))
    return pl.pallas_call(
        functools.partial(project_kernel, int(before is not None), 384),
        out_shape=jax.ShapeDtypeStruct((images, 2 * half, columns), BF),
        in_specs=[ANY] * len(arrays),
        out_specs=VMEM,
        scratch_shapes=[pltpu.VMEM(a.shape, BF) for a in arrays[:4]]
        + [pltpu.SemaphoreType.DMA((5,))],
        compiler_params=params(16),
        cost_estimate=cost(4 * images * half * width * weights.shape[1], 5 * 1024 * 1024),
        name="project" if before is None else "project_more",
    )(*arrays)


def output_kernel(part, features, w_own, w_other, out, rows, kept_own, kept_other, sems):
    images, half, width = rows.shape
    cols = kept_own.shape[1]
    copies = [
        pltpu.make_async_copy(
            features.at[:, part * half : (part + 1) * half], rows, sems.at[0]
        ),
        pltpu.make_async_copy(w_own, kept_own, sems.at[1]),
        pltpu.make_async_copy(w_other, kept_other, sems.at[2]),
    ]
    for copy in copies:
        copy.start()
    copies[0].wait()
    left = rows[...].reshape(images * half, width)
    for n, kept in enumerate((kept_own, kept_other)):
        copies[n + 1].wait()
        for m in range(2):
            at = slice(m * cols // 2, (m + 1) * cols // 2)
            value = dot(left, kept[:, at]).astype(out.dtype).reshape(images, half, cols // 2)
            out[:, :, n * cols + m * cols // 2 : n * cols + (m + 1) * cols // 2] = value


def output(features, w_own, w_other, part, kind):
    images, patches, width = features.shape
    half, cols = patches // 2, w_own.shape[1]
    return pl.pallas_call(
        functools.partial(output_kernel, part),
        out_shape=jax.ShapeDtypeStruct((images, half, 2 * cols), kind),
        in_specs=[ANY] * 3,
        out_specs=VMEM,
        scratch_shapes=[
            pltpu.VMEM((images, half, width), BF),
            pltpu.VMEM(w_own.shape, BF),
            pltpu.VMEM(w_other.shape, BF),
            pltpu.SemaphoreType.DMA((3,)),
        ],
        compiler_params=params(16),
        cost_estimate=cost(4 * images * half * width * cols, 4 * 1024 * 1024),
        name="output_sent" if part else "output_kept",
    )(features, w_own, w_other)


def finish_kernel(n_y, arrived, tokens, out):
    pieces, _, width = arrived.shape
    cols = width // 2
    lower = lax.axis_index("xl") == 0
    for y in range(n_y):
        at = slice(y * pieces // n_y, (y + 1) * pieces // n_y)
        total = arrived[at].astype(F32).sum(axis=0)
        left, right = total[:, :cols], total[:, cols:]
        for n, value in enumerate(
            (jnp.where(lower, left, right), jnp.where(lower, right, left))
        ):
            to = slice((n * n_y + y) * cols, (n * n_y + y + 1) * cols)
            out[:, to] = (tokens[:, to].astype(F32) + value).astype(BF)


def finish(arrived, tokens, n_y):
    return pl.pallas_call(
        functools.partial(finish_kernel, n_y),
        out_shape=jax.ShapeDtypeStruct(tokens.shape, BF),
        in_specs=[VMEM] * 2,
        out_specs=VMEM,
        compiler_params=params(8),
        cost_estimate=cost(arrived.size, 2 * 1024 * 1024),
        name="finish",
    )(arrived, tokens)


def block(
    tokens, norm_gain, w_query, w_key, w_value, w_inner, bias_inner, w_attn_out, w_outer, temper
):
    count = tokens.shape[0]
    n_y, n_z, n_xh = (lax.axis_size(a) for a in ("y", "z", "xh"))
    beside = partner(tokens, "xh")
    w_qkv = jnp.concatenate((w_query, w_key, w_value), axis=1)
    w_out = jnp.concatenate((w_attn_out, w_outer), axis=0)
    w_inner_p = partner(w_inner, "xl")
    w_qkv_p = partner(w_qkv, "xl")
    w_out_p = partner(w_out, "xl")
    pieces = spread(tokens, beside, norm_gain, n_y, n_z)
    mine = exchange(pieces, ("y", "z"))
    mine = mine.reshape(n_y, -1, mine.shape[-1])
    theirs = partner(mine, "c")
    partial = project(mine, theirs, w_inner, w_inner_p)
    partial = project(mine, theirs, w_qkv, w_qkv_p, partial)
    sums = exchange(partial, "y").astype(F32).sum(axis=0)
    scale = temper / math.sqrt(HEAD)
    query_norm = normalize(sums[:, :HEAD].astype(BF).astype(F32)).astype(BF)
    key_norm = normalize(sums[:, HEAD : 2 * HEAD].astype(BF).astype(F32)).astype(BF)
    value = sums[:, 2 * HEAD : 3 * HEAD].astype(BF)
    scores = jnp.einsum("qc,kc->qk", query_norm, key_norm, preferred_element_type=F32)
    scores = scores * scale
    probs = jax.nn.softmax(scores, axis=-1).astype(BF)
    mixed = dot(probs, value).astype(BF)
    inner = sums[:, 3 * HEAD :] + bias_inner
    activ = jax.nn.gelu(inner, approximate=False).astype(BF)
    features = jnp.concatenate((mixed, activ), axis=1)
    features = exchange(jnp.broadcast_to(features, (n_y, *features.shape)), "y")
    sent = partner(output(features, w_out, w_out_p, 1, BF), "c")
    kept = output(features, w_out, w_out_p, 0, F32)
    summed = (kept + sent.astype(F32)).astype(BF)
    pieces = summed.reshape(n_y * n_z * n_xh, count, summed.shape[-1])
    arrived = exchange(pieces, ("y", "z", "xh"))
    return finish(arrived, tokens, n_y)


def solution(mesh):
    finer = Mesh(mesh.devices.reshape(2, 4, 8, 2, 2), ALL)
    return jax.shard_map(
        block,
        mesh=finer,
        in_specs=(
            P(ALL, None),
            P(),
            P(DP, MP),
            P(DP, MP),
            P(DP, MP),
            P(DP, MP),
            P(MP),
            P(MP, DP),
            P(MP, DP),
            P(MP),
        ),
        out_specs=P(ALL, None),
        check_vma=False,
    )
```

```python
import functools
import math

import jax
import jax.numpy as jnp
from jax import lax
from jax.experimental import pallas as pl
from jax.experimental.pallas import tpu as pltpu
from jax.sharding import Mesh
from jax.sharding import PartitionSpec as P


HEAD = 128
DP = ("xl", "y")
MP = ("z", "xh", "c")
ALL = DP + MP
BF = jnp.bfloat16
F32 = jnp.float32
ANY = pl.BlockSpec(memory_space=pl.ANY)
VMEM = pl.BlockSpec(memory_space=pltpu.VMEM)


def normalize(values):
    center = values - jnp.mean(values, axis=-1, keepdims=True)
    spread = jnp.mean(center * center, axis=-1, keepdims=True)
    return center * lax.rsqrt(spread + 1e-06)


def partner(array, axis):
    return lax.ppermute(array, axis, [(0, 1), (1, 0)])


def exchange(pieces, axes):
    return lax.all_to_all(pieces, axes, split_axis=0, concat_axis=0, tiled=True)


def dot(a, b):
    return lax.dot_general(a, b, (((a.ndim - 1,), (0,)), ((), ())), preferred_element_type=F32)


def params(mib):
    return pltpu.CompilerParams(vmem_limit_bytes=mib * 1024 * 1024)


def cost(flops, moved):
    return pl.CostEstimate(flops=flops, bytes_accessed=moved, transcendentals=0)


def spread_kernel(n_y, n_z, tokens, received, norm_gain, out, own, beside, gain, sems):
    _, width = own.shape
    cols = width // (2 * n_y)
    copies = [
        pltpu.make_async_copy(tokens, own, sems.at[0]),
        pltpu.make_async_copy(received, beside, sems.at[1]),
        pltpu.make_async_copy(norm_gain, gain, sems.at[2]),
    ]
    for copy in copies:
        copy.start()
    for copy in copies:
        copy.wait()
    mine, theirs = own[...].astype(F32), beside[...].astype(F32)
    first = lax.axis_index("xh") == 0
    rows = jnp.concatenate(
        (jnp.where(first, mine, theirs), jnp.where(first, theirs, mine)), axis=0
    )
    normed = normalize(rows) * gain[...]
    lower = lax.axis_index("xl") == 0
    for y in range(n_y):
        a = normed[:, y * cols : (y + 1) * cols]
        b = normed[:, (n_y + y) * cols : (n_y + y + 1) * cols]
        left = jnp.where(lower, a, b).astype(BF)
        right = jnp.where(lower, b, a).astype(BF)
        for z in range(n_z):
            out[y * n_z + z, :, :cols] = left
            out[y * n_z + z, :, cols:] = right


def spread(tokens, beside, gain, n_y, n_z):
    count, width = tokens.shape
    return pl.pallas_call(
        functools.partial(spread_kernel, n_y, n_z),
        out_shape=jax.ShapeDtypeStruct((n_y * n_z, 2 * count, width // n_y), BF),
        in_specs=[ANY] * 3,
        out_specs=VMEM,
        scratch_shapes=[
            pltpu.VMEM((count, width), BF),
            pltpu.VMEM((count, width), BF),
            pltpu.VMEM((1, width), F32),
            pltpu.SemaphoreType.DMA((3,)),
        ],
        compiler_params=pltpu.CompilerParams(vmem_limit_bytes=67_000_000),
        cost_estimate=cost(20 * count * width, 2 * 1024 * 1024),
        name="normed_pieces",
    )(tokens, beside, gain.reshape(1, width))


def product(rows, w, w_p, at):
    cols = rows.shape[1] // 2
    return dot(rows[:, :cols], w[:, at]) + dot(rows[:, cols:], w_p[:, at])


def inner_kernel(tokens, w_own, w_other, out, rows, kept, kept_p, sems):
    copies = [
        pltpu.make_async_copy(tokens, rows, sems.at[0]),
        pltpu.make_async_copy(w_own, kept, sems.at[1]),
        pltpu.make_async_copy(w_other, kept_p, sems.at[2]),
    ]
    for copy in copies:
        copy.start()
    for copy in copies:
        copy.wait()
    images, half, width = rows.shape
    left = rows[...].reshape(images * half, width)
    for n in range(kept.shape[1] // 384):
        at = slice(n * 384, (n + 1) * 384)
        value = product(left, kept, kept_p, at)
        out[:, :, at] = value.astype(BF).reshape(images, half, 384)


def inner_part(tokens, w_own, w_other):
    images, half, width = tokens.shape
    columns = w_own.shape[1]
    return pl.pallas_call(
        inner_kernel,
        out_shape=jax.ShapeDtypeStruct((images, half, columns), BF),
        in_specs=[ANY, ANY, ANY],
        out_specs=VMEM,
        scratch_shapes=[
            pltpu.VMEM(tokens.shape, BF),
            pltpu.VMEM(w_own.shape, BF),
            pltpu.VMEM(w_other.shape, BF),
            pltpu.SemaphoreType.DMA((3,)),
        ],
        compiler_params=params(12),
        cost_estimate=cost(2 * images * half * width * columns, 4 * 1024 * 1024),
        name="inner_part",
    )(tokens, w_own, w_other)


def heads_kernel(
    mine, theirs, w_own, w_other, inner_mine, inner_theirs, out, rows, rows_p, kept, kept_p, sems
):
    images, half, width = rows.shape
    wide = w_own.shape[1]
    copies = [
        pltpu.make_async_copy(mine, rows, sems.at[0]),
        pltpu.make_async_copy(w_own, kept, sems.at[1]),
        pltpu.make_async_copy(w_other, kept_p, sems.at[2]),
        pltpu.make_async_copy(theirs, rows_p, sems.at[3]),
        pltpu.make_async_copy(inner_mine, out.at[:, :half, wide:], sems.at[4]),
        pltpu.make_async_copy(inner_theirs, out.at[:, half:, wide:], sems.at[5]),
    ]
    for copy in copies:
        copy.start()
    for copy in copies[:3]:
        copy.wait()
    for part, source in enumerate((rows, rows_p)):
        if part:
            copies[3].wait()
        left = source[...].reshape(images * half, width)
        value = product(left, kept, kept_p, slice(0, wide))
        out[:, part * half : (part + 1) * half, :wide] = value.astype(BF).reshape(
            images, half, wide
        )
    for copy in copies[4:]:
        copy.wait()


def heads_part(mine, theirs, w_own, w_other, inner_mine, inner_theirs):
    images, half, width = mine.shape
    wide = w_own.shape[1]
    return pl.pallas_call(
        heads_kernel,
        out_shape=jax.ShapeDtypeStruct((images, 2 * half, wide + inner_mine.shape[2]), BF),
        in_specs=[ANY, ANY, ANY, ANY, ANY, ANY],
        out_specs=VMEM,
        scratch_shapes=[pltpu.VMEM(mine.shape, BF)] * 2
        + [pltpu.VMEM(w_own.shape, BF)] * 2
        + [pltpu.SemaphoreType.DMA((6,))],
        compiler_params=params(12),
        cost_estimate=cost(4 * images * half * width * wide, 4 * 1024 * 1024),
        name="heads_part",
    )(mine, theirs, w_own, w_other, inner_mine, inner_theirs)


def middle_kernel(arrived, bias, scale, out, kept, sem):
    copy = pltpu.make_async_copy(bias, kept, sem)
    copy.start()
    copies, columns = out.shape[0], kept.shape[0]

    def summed(at):
        total = arrived[0, :, at].astype(F32)
        for n in range(1, arrived.shape[0]):
            total = total + arrived[n, :, at].astype(F32)
        return total

    def rounded(n):
        return summed(slice(n * HEAD, (n + 1) * HEAD)).astype(BF)

    query_norm = normalize(rounded(0).astype(F32)).astype(BF)
    key_norm = normalize(rounded(1).astype(F32)).astype(BF)
    scores = lax.dot_general(
        query_norm, key_norm, (((1,), (1,)), ((), ())), preferred_element_type=F32
    )
    scores = scores * scale[0]
    powers = jnp.exp(scores - jnp.max(scores, axis=-1, keepdims=True))
    probs = (powers / jnp.sum(powers, axis=-1, keepdims=True)).astype(BF)
    mixed = dot(probs, rounded(2)).astype(BF)
    for n in range(copies):
        out[n, :, :HEAD] = mixed
    copy.wait()
    for m in range(columns // 256):
        at = slice(m * 256, (m + 1) * 256)
        inner = summed(slice(3 * HEAD + m * 256, 3 * HEAD + (m + 1) * 256)) + kept[at]
        activ = (inner * (0.5 + 0.5 * lax.erf(inner * math.sqrt(0.5)))).astype(BF)
        for n in range(copies):
            out[n, :, HEAD + m * 256 : HEAD + (m + 1) * 256] = activ


def middle(arrived, bias, scale):
    copies, patches, _ = arrived.shape
    columns = bias.shape[0]
    return pl.pallas_call(
        middle_kernel,
        out_shape=jax.ShapeDtypeStruct((copies, patches, HEAD + columns), BF),
        in_specs=[VMEM, ANY, pl.BlockSpec(memory_space=pltpu.SMEM)],
        out_specs=VMEM,
        scratch_shapes=[pltpu.VMEM((columns,), F32), pltpu.SemaphoreType.DMA],
        compiler_params=params(12),
        cost_estimate=cost(60 * patches * columns, 2 * 1024 * 1024),
        name="middle",
    )(arrived, bias, scale)


def output_kernel(part, features, *refs):
    sources, out, rows, kept, sems = refs[:4], refs[4], refs[5], refs[6:8], refs[8]
    images, half, width = rows.shape
    heads = sources[0].shape[0]
    cols = kept[0].shape[1]
    first = pltpu.make_async_copy(
        features.at[:, part * half : (part + 1) * half], rows, sems.at[4]
    )
    copies = []
    for n, source in enumerate(sources):
        to = kept[n // 2].at[pl.ds(heads, width - heads) if n % 2 else pl.ds(0, heads)]
        copies.append(pltpu.make_async_copy(source, to, sems.at[n]))
    first.start()
    for copy in copies:
        copy.start()
    first.wait()
    left = rows[...].reshape(images * half, width)
    for n in range(2):
        copies[2 * n].wait()
        copies[2 * n + 1].wait()
        for m in range(2):
            at = slice(m * cols // 2, (m + 1) * cols // 2)
            value = dot(left, kept[n][:, at]).astype(out.dtype)
            to = slice(n * cols + m * cols // 2, n * cols + (m + 1) * cols // 2)
            out[:, :, to] = value.reshape(images, half, cols // 2)


def output(features, weights, part, kind):
    images, patches, width = features.shape
    half, cols = patches // 2, weights[0].shape[1]
    return pl.pallas_call(
        functools.partial(output_kernel, part),
        out_shape=jax.ShapeDtypeStruct((images, half, 2 * cols), kind),
        in_specs=[ANY] * 5,
        out_specs=VMEM,
        scratch_shapes=[pltpu.VMEM((images, half, width), BF)]
        + [pltpu.VMEM((width, cols), BF)] * 2
        + [pltpu.SemaphoreType.DMA((5,))],
        compiler_params=params(16),
        cost_estimate=cost(4 * images * half * width * cols, 4 * 1024 * 1024),
        name="output_sent" if part else "output_kept",
    )(features, *weights)


def finish_kernel(n_y, arrived, tokens, out):
    pieces, _, width = arrived.shape
    cols = width // 2
    lower = lax.axis_index("xl") == 0
    for y in range(n_y):
        at = slice(y * pieces // n_y, (y + 1) * pieces // n_y)
        total = arrived[at].astype(F32).sum(axis=0)
        left, right = total[:, :cols], total[:, cols:]
        for n, value in enumerate(
            (jnp.where(lower, left, right), jnp.where(lower, right, left))
        ):
            to = slice((n * n_y + y) * cols, (n * n_y + y + 1) * cols)
            out[:, to] = (tokens[:, to].astype(F32) + value).astype(BF)


def finish(arrived, tokens, n_y):
    return pl.pallas_call(
        functools.partial(finish_kernel, n_y),
        out_shape=jax.ShapeDtypeStruct(tokens.shape, BF),
        in_specs=[VMEM] * 2,
        out_specs=VMEM,
        compiler_params=params(8),
        cost_estimate=cost(arrived.size, 2 * 1024 * 1024),
        name="finish",
    )(arrived, tokens)


def block(
    tokens, norm_gain, w_query, w_key, w_value, w_inner, bias_inner, w_attn_out, w_outer, temper
):
    count = tokens.shape[0]
    n_y, n_z, n_xh = (lax.axis_size(a) for a in ("y", "z", "xh"))
    beside = partner(tokens, "xh")
    w_qkv = jnp.concatenate((w_query, w_key, w_value), axis=1)
    w_inner_p = partner(w_inner, "xl")
    w_qkv_p = partner(w_qkv, "xl")
    w_attn_out_p = partner(w_attn_out, "xl")
    w_outer_p = partner(w_outer, "xl")
    pieces = spread(tokens, beside, norm_gain, n_y, n_z)
    mine = exchange(pieces, ("y", "z"))
    mine = mine.reshape(n_y, -1, mine.shape[-1])
    theirs = partner(mine, "c")
    inner_mine = inner_part(mine, w_inner, w_inner_p)
    inner_theirs = inner_part(theirs, w_inner, w_inner_p)
    partial = heads_part(mine, theirs, w_qkv, w_qkv_p, inner_mine, inner_theirs)
    arrived = exchange(partial, "y")
    scale = temper / math.sqrt(HEAD)
    features = middle(arrived, bias_inner, scale)
    features, w_attn_out_p, w_outer_p = lax.optimization_barrier(
        (features, w_attn_out_p, w_outer_p)
    )
    w_out = (w_attn_out, w_outer, w_attn_out_p, w_outer_p)
    features = exchange(features, "y")
    sent = partner(output(features, w_out, 1, BF), "c")
    kept = output(features, w_out, 0, F32)
    summed = (kept + sent.astype(F32)).astype(BF)
    pieces = summed.reshape(n_y * n_z * n_xh, count, summed.shape[-1])
    arrived = exchange(pieces, ("y", "z", "xh"))
    return finish(arrived, tokens, n_y)


def solution(mesh):
    finer = Mesh(mesh.devices.reshape(2, 4, 8, 2, 2), ALL)
    return jax.shard_map(
        block,
        mesh=finer,
        in_specs=(
            P(ALL, None),
            P(),
            P(DP, MP),
            P(DP, MP),
            P(DP, MP),
            P(DP, MP),
            P(MP),
            P(MP, DP),
            P(MP, DP),
            P(MP),
        ),
        out_specs=P(ALL, None),
        check_vma=False,
    )
```

```python
import functools
import math

import jax
import jax.numpy as jnp
from jax import lax
from jax.experimental import pallas as pl
from jax.experimental.pallas import tpu as pltpu
from jax.sharding import Mesh
from jax.sharding import PartitionSpec as P


HEAD = 128
DP = ("xl", "y")
MP = ("z", "xh", "c")
ALL = DP + MP
BF = jnp.bfloat16
F32 = jnp.float32
ANY = pl.BlockSpec(memory_space=pl.ANY)
VMEM = pl.BlockSpec(memory_space=pltpu.VMEM)


def normalize(values):
    center = values - jnp.mean(values, axis=-1, keepdims=True)
    spread = jnp.mean(center * center, axis=-1, keepdims=True)
    return center * lax.rsqrt(spread + 1e-06)


def partner(array, axis):
    return lax.ppermute(array, axis, [(0, 1), (1, 0)])


def exchange(pieces, axes):
    return lax.all_to_all(pieces, axes, split_axis=0, concat_axis=0, tiled=True)


def dot(a, b):
    return lax.dot_general(a, b, (((a.ndim - 1,), (0,)), ((), ())), preferred_element_type=F32)


def params(mib):
    return pltpu.CompilerParams(vmem_limit_bytes=mib * 1024 * 1024)


def cost(flops, moved):
    return pl.CostEstimate(flops=flops, bytes_accessed=moved, transcendentals=0)


def spread_kernel(n_y, n_z, tokens, received, norm_gain, out, own, beside, gain, sems):
    _, width = own.shape
    cols = width // (2 * n_y)
    copies = [
        pltpu.make_async_copy(tokens, own, sems.at[0]),
        pltpu.make_async_copy(received, beside, sems.at[1]),
        pltpu.make_async_copy(norm_gain, gain, sems.at[2]),
    ]
    for copy in copies:
        copy.start()
    for copy in copies:
        copy.wait()
    mine, theirs = own[...].astype(F32), beside[...].astype(F32)
    first = lax.axis_index("xh") == 0
    rows = jnp.concatenate(
        (jnp.where(first, mine, theirs), jnp.where(first, theirs, mine)), axis=0
    )
    normed = normalize(rows) * gain[...]
    lower = lax.axis_index("xl") == 0
    for y in range(n_y):
        a = normed[:, y * cols : (y + 1) * cols]
        b = normed[:, (n_y + y) * cols : (n_y + y + 1) * cols]
        left = jnp.where(lower, a, b).astype(BF)
        right = jnp.where(lower, b, a).astype(BF)
        for z in range(n_z):
            out[y * n_z + z, :, :cols] = left
            out[y * n_z + z, :, cols:] = right


def spread(tokens, beside, gain, n_y, n_z):
    count, width = tokens.shape
    return pl.pallas_call(
        functools.partial(spread_kernel, n_y, n_z),
        out_shape=jax.ShapeDtypeStruct((n_y * n_z, 2 * count, width // n_y), BF),
        in_specs=[ANY] * 3,
        out_specs=VMEM,
        scratch_shapes=[
            pltpu.VMEM((count, width), BF),
            pltpu.VMEM((count, width), BF),
            pltpu.VMEM((1, width), F32),
            pltpu.SemaphoreType.DMA((3,)),
        ],
        compiler_params=pltpu.CompilerParams(vmem_limit_bytes=67_000_000),
        cost_estimate=cost(20 * count * width, 2 * 1024 * 1024),
        name="normed_pieces",
    )(tokens, beside, gain.reshape(1, width))


def product(rows, w, w_p, at):
    cols = rows.shape[1] // 2
    return dot(rows[:, :cols], w[:, at]) + dot(rows[:, cols:], w_p[:, at])


def inner_kernel(tokens, w_own, w_other, out, rows, kept, kept_p, sems):
    copies = [
        pltpu.make_async_copy(tokens, rows, sems.at[0]),
        pltpu.make_async_copy(w_own, kept, sems.at[1]),
        pltpu.make_async_copy(w_other, kept_p, sems.at[2]),
    ]
    for copy in copies:
        copy.start()
    for copy in copies:
        copy.wait()
    images, half, width = rows.shape
    left = rows[...].reshape(images * half, width)
    for n in range(kept.shape[1] // 384):
        at = slice(n * 384, (n + 1) * 384)
        value = product(left, kept, kept_p, at)
        out[:, :, at] = value.astype(BF).reshape(images, half, 384)


def inner_part(tokens, w_own, w_other):
    images, half, width = tokens.shape
    columns = w_own.shape[1]
    return pl.pallas_call(
        inner_kernel,
        out_shape=jax.ShapeDtypeStruct((images, half, columns), BF),
        in_specs=[ANY, ANY, ANY],
        out_specs=VMEM,
        scratch_shapes=[
            pltpu.VMEM(tokens.shape, BF),
            pltpu.VMEM(w_own.shape, BF),
            pltpu.VMEM(w_other.shape, BF),
            pltpu.SemaphoreType.DMA((3,)),
        ],
        compiler_params=params(12),
        cost_estimate=cost(2 * images * half * width * columns, 4 * 1024 * 1024),
        name="inner_part",
    )(tokens, w_own, w_other)


def heads_kernel(
    mine, theirs, w_own, w_other, inner_mine, inner_theirs, out, rows, rows_p, kept, kept_p, sems
):
    images, half, width = rows.shape
    wide = w_own.shape[1]
    copies = [
        pltpu.make_async_copy(mine, rows, sems.at[0]),
        pltpu.make_async_copy(w_own, kept, sems.at[1]),
        pltpu.make_async_copy(w_other, kept_p, sems.at[2]),
        pltpu.make_async_copy(theirs, rows_p, sems.at[3]),
        pltpu.make_async_copy(inner_mine, out.at[:, :half, wide:], sems.at[4]),
        pltpu.make_async_copy(inner_theirs, out.at[:, half:, wide:], sems.at[5]),
    ]
    for copy in copies:
        copy.start()
    for copy in copies[:3]:
        copy.wait()
    for part, source in enumerate((rows, rows_p)):
        if part:
            copies[3].wait()
        left = source[...].reshape(images * half, width)
        value = product(left, kept, kept_p, slice(0, wide))
        out[:, part * half : (part + 1) * half, :wide] = value.astype(BF).reshape(
            images, half, wide
        )
    for copy in copies[4:]:
        copy.wait()


def heads_part(mine, theirs, w_own, w_other, inner_mine, inner_theirs):
    images, half, width = mine.shape
    wide = w_own.shape[1]
    return pl.pallas_call(
        heads_kernel,
        out_shape=jax.ShapeDtypeStruct((images, 2 * half, wide + inner_mine.shape[2]), BF),
        in_specs=[ANY, ANY, ANY, ANY, ANY, ANY],
        out_specs=VMEM,
        scratch_shapes=[pltpu.VMEM(mine.shape, BF)] * 2
        + [pltpu.VMEM(w_own.shape, BF)] * 2
        + [pltpu.SemaphoreType.DMA((6,))],
        compiler_params=params(12),
        cost_estimate=cost(4 * images * half * width * wide, 4 * 1024 * 1024),
        name="heads_part",
    )(mine, theirs, w_own, w_other, inner_mine, inner_theirs)


def middle_kernel(arrived, bias, scale, out, kept, sem):
    copy = pltpu.make_async_copy(bias, kept, sem)
    copy.start()
    copies, columns = out.shape[0], kept.shape[0]

    def summed(at):
        total = arrived[0, :, at].astype(F32)
        for n in range(1, arrived.shape[0]):
            total = total + arrived[n, :, at].astype(F32)
        return total

    def rounded(n):
        return summed(slice(n * HEAD, (n + 1) * HEAD)).astype(BF)

    query_norm = normalize(rounded(0).astype(F32)).astype(BF)
    key_norm = normalize(rounded(1).astype(F32)).astype(BF)
    scores = lax.dot_general(
        query_norm, key_norm, (((1,), (1,)), ((), ())), preferred_element_type=F32
    )
    scores = scores * scale[0]
    powers = jnp.exp(scores - jnp.max(scores, axis=-1, keepdims=True))
    probs = (powers / jnp.sum(powers, axis=-1, keepdims=True)).astype(BF)
    mixed = dot(probs, rounded(2)).astype(BF)
    for n in range(copies):
        out[n, :, :HEAD] = mixed
    copy.wait()
    for m in range(columns // 256):
        at = slice(m * 256, (m + 1) * 256)
        inner = summed(slice(3 * HEAD + m * 256, 3 * HEAD + (m + 1) * 256)) + kept[at]
        activ = (inner * (0.5 + 0.5 * lax.erf(inner * math.sqrt(0.5)))).astype(BF)
        for n in range(copies):
            out[n, :, HEAD + m * 256 : HEAD + (m + 1) * 256] = activ


def middle(arrived, bias, scale):
    _, patches, _ = arrived.shape
    columns = bias.shape[0]
    return pl.pallas_call(
        middle_kernel,
        out_shape=jax.ShapeDtypeStruct((1, patches, HEAD + columns), BF),
        in_specs=[VMEM, ANY, pl.BlockSpec(memory_space=pltpu.SMEM)],
        out_specs=VMEM,
        scratch_shapes=[pltpu.VMEM((columns,), F32), pltpu.SemaphoreType.DMA],
        compiler_params=params(12),
        cost_estimate=cost(60 * patches * columns, 2 * 1024 * 1024),
        name="middle",
    )(arrived, bias, scale)


def output_kernel(part, features, w_own, w_other, out, rows, kept_own, kept_other, sems):
    images, half, width = rows.shape
    cols = kept_own.shape[1]
    copies = [
        pltpu.make_async_copy(
            features.at[:, part * half : (part + 1) * half], rows, sems.at[0]
        ),
        pltpu.make_async_copy(w_own, kept_own, sems.at[1]),
        pltpu.make_async_copy(w_other, kept_other, sems.at[2]),
    ]
    for copy in copies:
        copy.start()
    copies[0].wait()
    left = rows[...].reshape(images * half, width)
    for n, kept in enumerate((kept_own, kept_other)):
        copies[n + 1].wait()
        for m in range(2):
            at = slice(m * cols // 2, (m + 1) * cols // 2)
            value = dot(left, kept[:, at]).astype(out.dtype).reshape(images, half, cols // 2)
            out[:, :, n * cols + m * cols // 2 : n * cols + (m + 1) * cols // 2] = value


def output(features, w_own, w_other, part, kind):
    images, patches, width = features.shape
    half, cols = patches // 2, w_own.shape[1]
    return pl.pallas_call(
        functools.partial(output_kernel, part),
        out_shape=jax.ShapeDtypeStruct((images, half, 2 * cols), kind),
        in_specs=[ANY] * 3,
        out_specs=VMEM,
        scratch_shapes=[
            pltpu.VMEM((images, half, width), BF),
            pltpu.VMEM(w_own.shape, BF),
            pltpu.VMEM(w_other.shape, BF),
            pltpu.SemaphoreType.DMA((3,)),
        ],
        compiler_params=params(16),
        cost_estimate=cost(4 * images * half * width * cols, 4 * 1024 * 1024),
        name="output_sent" if part else "output_kept",
    )(features, w_own, w_other)


def finish_kernel(n_y, arrived, tokens, out):
    pieces, _, width = arrived.shape
    cols = width // 2
    lower = lax.axis_index("xl") == 0
    for y in range(n_y):
        at = slice(y * pieces // n_y, (y + 1) * pieces // n_y)
        total = arrived[at].astype(F32).sum(axis=0)
        left, right = total[:, :cols], total[:, cols:]
        for n, value in enumerate(
            (jnp.where(lower, left, right), jnp.where(lower, right, left))
        ):
            to = slice((n * n_y + y) * cols, (n * n_y + y + 1) * cols)
            out[:, to] = (tokens[:, to].astype(F32) + value).astype(BF)


def finish(arrived, tokens, n_y):
    return pl.pallas_call(
        functools.partial(finish_kernel, n_y),
        out_shape=jax.ShapeDtypeStruct(tokens.shape, BF),
        in_specs=[VMEM] * 2,
        out_specs=VMEM,
        compiler_params=params(8),
        cost_estimate=cost(arrived.size, 2 * 1024 * 1024),
        name="finish",
    )(arrived, tokens)


def block(
    tokens, norm_gain, w_query, w_key, w_value, w_inner, bias_inner, w_attn_out, w_outer, temper
):
    count = tokens.shape[0]
    n_y, n_z, n_xh = (lax.axis_size(a) for a in ("y", "z", "xh"))
    beside = partner(tokens, "xh")
    w_qkv = jnp.concatenate((w_query, w_key, w_value), axis=1)
    w_inner_p = partner(w_inner, "xl")
    w_qkv_p = partner(w_qkv, "xl")
    w_out = jnp.concatenate((w_attn_out, w_outer), axis=0)
    w_out_p = partner(w_out, "xl")
    pieces = spread(tokens, beside, norm_gain, n_y, n_z)
    mine = exchange(pieces, ("y", "z"))
    mine = mine.reshape(n_y, -1, mine.shape[-1])
    theirs = partner(mine, "c")
    inner_mine = inner_part(mine, w_inner, w_inner_p)
    inner_theirs = inner_part(theirs, w_inner, w_inner_p)
    partial = heads_part(mine, theirs, w_qkv, w_qkv_p, inner_mine, inner_theirs)
    arrived = exchange(partial, "y")
    scale = temper / math.sqrt(HEAD)
    features = middle(arrived, bias_inner, scale)[0]
    features = lax.all_gather(features, "y", axis=0, tiled=False)
    sent = partner(output(features, w_out, w_out_p, 1, BF), "c")
    kept = output(features, w_out, w_out_p, 0, F32)
    summed = (kept + sent.astype(F32)).astype(BF)
    pieces = summed.reshape(n_y * n_z * n_xh, count, summed.shape[-1])
    arrived = exchange(pieces, ("y", "z", "xh"))
    return finish(arrived, tokens, n_y)


def solution(mesh):
    finer = Mesh(mesh.devices.reshape(2, 4, 8, 2, 2), ALL)
    return jax.shard_map(
        block,
        mesh=finer,
        in_specs=(
            P(ALL, None),
            P(),
            P(DP, MP),
            P(DP, MP),
            P(DP, MP),
            P(DP, MP),
            P(MP),
            P(MP, DP),
            P(MP, DP),
            P(MP),
        ),
        out_specs=P(ALL, None),
        check_vma=False,
    )
```

```python
import functools
import math

import jax
import jax.numpy as jnp
from jax import lax
from jax.experimental import pallas as pl
from jax.experimental.pallas import tpu as pltpu
from jax.sharding import Mesh
from jax.sharding import PartitionSpec as P


HEAD = 128
DP = ("xl", "y")
MP = ("z", "xh", "c")
ALL = DP + MP
BF = jnp.bfloat16
F32 = jnp.float32
ANY = pl.BlockSpec(memory_space=pl.ANY)
VMEM = pl.BlockSpec(memory_space=pltpu.VMEM)


def normalize(values):
    center = values - jnp.mean(values, axis=-1, keepdims=True)
    spread = jnp.mean(center * center, axis=-1, keepdims=True)
    return center * lax.rsqrt(spread + 1e-06)


def partner(array, axis):
    return lax.ppermute(array, axis, [(0, 1), (1, 0)])


def exchange(pieces, axes):
    return lax.all_to_all(pieces, axes, split_axis=0, concat_axis=0, tiled=True)


def dot(a, b):
    return lax.dot_general(a, b, (((a.ndim - 1,), (0,)), ((), ())), preferred_element_type=F32)


def params(mib):
    return pltpu.CompilerParams(vmem_limit_bytes=mib * 1024 * 1024)


def cost(flops, moved):
    return pl.CostEstimate(flops=flops, bytes_accessed=moved, transcendentals=0)


def norm_kernel(tokens, norm_gain, normed, gain, own, sems):
    copies = [
        pltpu.make_async_copy(tokens, own, sems.at[0]),
        pltpu.make_async_copy(norm_gain, gain, sems.at[1]),
    ]
    for copy in copies:
        copy.start()
    copies[0].wait()
    values = normalize(own[...].astype(F32))
    copies[1].wait()
    normed[...] = values * gain[...]


def norm_own(tokens, gain):
    count, width = tokens.shape
    return pl.pallas_call(
        norm_kernel,
        out_shape=(
            jax.ShapeDtypeStruct((count, width), F32),
            jax.ShapeDtypeStruct((1, width), F32),
        ),
        in_specs=[ANY] * 2,
        out_specs=(VMEM, VMEM),
        scratch_shapes=[pltpu.VMEM((count, width), BF), pltpu.SemaphoreType.DMA((2,))],
        compiler_params=params(8),
        cost_estimate=cost(100 * count * width, 1024 * 1024),
        name="norm_own",
    )(tokens, gain.reshape(1, width))


def spread_kernel(n_y, n_z, normed_own, gain, beside, out):
    _, width = beside.shape
    cols = width // (2 * n_y)
    mine = normed_own[...]
    theirs = normalize(beside[...].astype(F32)) * gain[...]
    first = lax.axis_index("xh") == 0
    normed = jnp.concatenate(
        (jnp.where(first, mine, theirs), jnp.where(first, theirs, mine)), axis=0
    )
    lower = lax.axis_index("xl") == 0
    for y in range(n_y):
        a = normed[:, y * cols : (y + 1) * cols]
        b = normed[:, (n_y + y) * cols : (n_y + y + 1) * cols]
        left = jnp.where(lower, a, b).astype(BF)
        right = jnp.where(lower, b, a).astype(BF)
        for z in range(n_z):
            out[y * n_z + z, :, :cols] = left
            out[y * n_z + z, :, cols:] = right


def spread(normed_own, gain, beside, n_y, n_z):
    count, width = beside.shape
    return pl.pallas_call(
        functools.partial(spread_kernel, n_y, n_z),
        out_shape=jax.ShapeDtypeStruct((n_y * n_z, 2 * count, width // n_y), BF),
        in_specs=[VMEM] * 3,
        out_specs=VMEM,
        compiler_params=params(8),
        cost_estimate=cost(20 * count * width, 2 * 1024 * 1024),
        name="normed_pieces",
    )(normed_own, gain, beside)


def product(rows, w, w_p, at):
    cols = rows.shape[1] // 2
    return dot(rows[:, :cols], w[:, at]) + dot(rows[:, cols:], w_p[:, at])


def inner_kernel(tokens, w_own, w_other, out, rows, kept, kept_p, sems):
    images, half, width = rows.shape
    chunk = 384
    first = pltpu.make_async_copy(tokens, rows, sems.at[0])
    copies = []
    for n in range(kept.shape[1] // chunk):
        at = pl.ds(n * chunk, chunk)
        for m, (source, to) in enumerate(((w_own, kept), (w_other, kept_p))):
            copies.append(
                pltpu.make_async_copy(source.at[:, at], to.at[:, at], sems.at[1 + 2 * n + m])
            )
    copies[0].start()
    first.start()
    for copy in copies[1:]:
        copy.start()
    first.wait()
    left = rows[...].reshape(images * half, width)
    for n in range(kept.shape[1] // chunk):
        copies[2 * n].wait()
        copies[2 * n + 1].wait()
        at = slice(n * chunk, (n + 1) * chunk)
        value = product(left, kept, kept_p, at)
        out[:, :, at] = value.astype(BF).reshape(images, half, chunk)


def inner_part(tokens, w_own, w_other):
    images, half, width = tokens.shape
    columns = w_own.shape[1]
    return pl.pallas_call(
        inner_kernel,
        out_shape=jax.ShapeDtypeStruct((images, half, columns), BF),
        in_specs=[ANY, ANY, ANY],
        out_specs=VMEM,
        scratch_shapes=[
            pltpu.VMEM(tokens.shape, BF),
            pltpu.VMEM(w_own.shape, BF),
            pltpu.VMEM(w_other.shape, BF),
            pltpu.SemaphoreType.DMA((5,)),
        ],
        compiler_params=params(12),
        cost_estimate=cost(2 * images * half * width * columns, 4 * 1024 * 1024),
        name="inner_part",
    )(tokens, w_own, w_other)


def heads_kernel(
    mine, theirs, w_own, w_other, inner_mine, inner_theirs, out, rows, rows_p, kept, kept_p, sems
):
    images, half, width = rows.shape
    wide = w_own.shape[1]
    copies = [
        pltpu.make_async_copy(mine, rows, sems.at[0]),
        pltpu.make_async_copy(w_own, kept, sems.at[1]),
        pltpu.make_async_copy(w_other, kept_p, sems.at[2]),
        pltpu.make_async_copy(theirs, rows_p, sems.at[3]),
        pltpu.make_async_copy(inner_mine, out.at[:, :half, wide:], sems.at[4]),
        pltpu.make_async_copy(inner_theirs, out.at[:, half:, wide:], sems.at[5]),
    ]
    for copy in copies:
        copy.start()
    cols = width // 2
    copies[0].wait()
    copies[1].wait()
    left = rows[...].reshape(images * half, width)
    own = dot(left[:, :cols], kept[...])
    copies[2].wait()
    out[:, :half, :wide] = (
        (own + dot(left[:, cols:], kept_p[...])).astype(BF).reshape(images, half, wide)
    )
    copies[3].wait()
    left = rows_p[...].reshape(images * half, width)
    value = dot(left[:, :cols], kept[...]) + dot(left[:, cols:], kept_p[...])
    out[:, half:, :wide] = value.astype(BF).reshape(images, half, wide)
    for copy in copies[4:]:
        copy.wait()


def heads_part(mine, theirs, w_own, w_other, inner_mine, inner_theirs):
    images, half, width = mine.shape
    wide = w_own.shape[1]
    return pl.pallas_call(
        heads_kernel,
        out_shape=jax.ShapeDtypeStruct((images, 2 * half, wide + inner_mine.shape[2]), BF),
        in_specs=[ANY, ANY, ANY, ANY, ANY, ANY],
        out_specs=VMEM,
        scratch_shapes=[pltpu.VMEM(mine.shape, BF)] * 2
        + [pltpu.VMEM(w_own.shape, BF)] * 2
        + [pltpu.SemaphoreType.DMA((6,))],
        compiler_params=params(12),
        cost_estimate=cost(4 * images * half * width * wide, 4 * 1024 * 1024),
        name="heads_part",
    )(mine, theirs, w_own, w_other, inner_mine, inner_theirs)


def middle_kernel(arrived, bias, scale, out, kept, sem):
    copy = pltpu.make_async_copy(bias, kept, sem)
    copy.start()
    copies, columns = out.shape[0], kept.shape[0]

    def summed(at):
        total = arrived[0, :, at].astype(F32)
        for n in range(1, arrived.shape[0]):
            total = total + arrived[n, :, at].astype(F32)
        return total

    def rounded(n):
        return summed(slice(n * HEAD, (n + 1) * HEAD)).astype(BF)

    query_norm = normalize(rounded(0).astype(F32)).astype(BF)
    key_norm = normalize(rounded(1).astype(F32)).astype(BF)
    scores = lax.dot_general(
        query_norm, key_norm, (((1,), (1,)), ((), ())), preferred_element_type=F32
    )
    scores = scores * scale[0]
    powers = jnp.exp(scores - jnp.max(scores, axis=-1, keepdims=True))
    probs = (powers / jnp.sum(powers, axis=-1, keepdims=True)).astype(BF)
    mixed = dot(probs, rounded(2)).astype(BF)
    for n in range(copies):
        out[n, :, :HEAD] = mixed
    copy.wait()
    for m in range(columns // 256):
        at = slice(m * 256, (m + 1) * 256)
        inner = summed(slice(3 * HEAD + m * 256, 3 * HEAD + (m + 1) * 256)) + kept[at]
        activ = (inner * (0.5 + 0.5 * lax.erf(inner * math.sqrt(0.5)))).astype(BF)
        for n in range(copies):
            out[n, :, HEAD + m * 256 : HEAD + (m + 1) * 256] = activ


def middle(arrived, bias, scale):
    _, patches, _ = arrived.shape
    columns = bias.shape[0]
    return pl.pallas_call(
        middle_kernel,
        out_shape=jax.ShapeDtypeStruct((1, patches, HEAD + columns), BF),
        in_specs=[VMEM, ANY, pl.BlockSpec(memory_space=pltpu.SMEM)],
        out_specs=VMEM,
        scratch_shapes=[pltpu.VMEM((columns,), F32), pltpu.SemaphoreType.DMA],
        compiler_params=params(12),
        cost_estimate=cost(60 * patches * columns, 2 * 1024 * 1024),
        name="middle",
    )(arrived, bias, scale)


def output_kernel(part, features, w_own, w_other, out, rows, kept_own, kept_other, sems):
    images, half, width = rows.shape
    cols = kept_own.shape[1]
    copies = [
        pltpu.make_async_copy(
            features.at[:, part * half : (part + 1) * half], rows, sems.at[0]
        ),
        pltpu.make_async_copy(w_own, kept_own, sems.at[1]),
        pltpu.make_async_copy(w_other, kept_other, sems.at[2]),
    ]
    for copy in copies:
        copy.start()
    copies[0].wait()
    left = rows[...].reshape(images * half, width)
    for n, kept in enumerate((kept_own, kept_other)):
        copies[n + 1].wait()
        for m in range(2):
            at = slice(m * cols // 2, (m + 1) * cols // 2)
            value = dot(left, kept[:, at]).astype(out.dtype).reshape(images, half, cols // 2)
            out[:, :, n * cols + m * cols // 2 : n * cols + (m + 1) * cols // 2] = value


def output(features, w_own, w_other, part, kind):
    images, patches, width = features.shape
    half, cols = patches // 2, w_own.shape[1]
    return pl.pallas_call(
        functools.partial(output_kernel, part),
        out_shape=jax.ShapeDtypeStruct((images, half, 2 * cols), kind),
        in_specs=[ANY] * 3,
        out_specs=VMEM,
        scratch_shapes=[
            pltpu.VMEM((images, half, width), BF),
            pltpu.VMEM(w_own.shape, BF),
            pltpu.VMEM(w_other.shape, BF),
            pltpu.SemaphoreType.DMA((3,)),
        ],
        compiler_params=params(16),
        cost_estimate=cost(4 * images * half * width * cols, 4 * 1024 * 1024),
        name="output_sent" if part else "output_kept",
    )(features, w_own, w_other)


def finish_kernel(n_y, arrived, tokens, out):
    pieces, _, width = arrived.shape
    cols = width // 2
    lower = lax.axis_index("xl") == 0
    for y in range(n_y):
        at = slice(y * pieces // n_y, (y + 1) * pieces // n_y)
        total = arrived[at].astype(F32).sum(axis=0)
        left, right = total[:, :cols], total[:, cols:]
        for n, value in enumerate(
            (jnp.where(lower, left, right), jnp.where(lower, right, left))
        ):
            to = slice((n * n_y + y) * cols, (n * n_y + y + 1) * cols)
            out[:, to] = (tokens[:, to].astype(F32) + value).astype(BF)


def finish(arrived, tokens, n_y):
    return pl.pallas_call(
        functools.partial(finish_kernel, n_y),
        out_shape=jax.ShapeDtypeStruct(tokens.shape, BF),
        in_specs=[VMEM] * 2,
        out_specs=VMEM,
        compiler_params=params(8),
        cost_estimate=cost(arrived.size, 2 * 1024 * 1024),
        name="finish",
    )(arrived, tokens)


def block(
    tokens, norm_gain, w_query, w_key, w_value, w_inner, bias_inner, w_attn_out, w_outer, temper
):
    count = tokens.shape[0]
    n_y, n_z, n_xh = (lax.axis_size(a) for a in ("y", "z", "xh"))
    beside = partner(tokens, "xh")
    w_qkv = jnp.concatenate((w_query, w_key, w_value), axis=1)
    w_inner_p = partner(w_inner, "xl")
    w_qkv_p = partner(w_qkv, "xl")
    w_out = jnp.concatenate((w_attn_out, w_outer), axis=0)
    w_out_p = partner(w_out, "xl")
    normed, gain = norm_own(tokens, norm_gain)
    pieces = spread(normed, gain, beside, n_y, n_z)
    mine = exchange(pieces, ("y", "z"))
    mine = mine.reshape(n_y, -1, mine.shape[-1])
    theirs = partner(mine, "c")
    inner_mine = inner_part(mine, w_inner, w_inner_p)
    inner_theirs = inner_part(theirs, w_inner, w_inner_p)
    partial = heads_part(mine, theirs, w_qkv, w_qkv_p, inner_mine, inner_theirs)
    arrived = exchange(partial, "y")
    scale = temper / math.sqrt(HEAD)
    features = middle(arrived, bias_inner, scale)[0]
    features = lax.all_gather(features, "y", axis=0, tiled=False)
    sent = partner(output(features, w_out, w_out_p, 1, BF), "c")
    kept = output(features, w_out, w_out_p, 0, F32)
    summed = (kept + sent.astype(F32)).astype(BF)
    pieces = summed.reshape(n_y * n_z * n_xh, count, summed.shape[-1])
    arrived = exchange(pieces, ("y", "z", "xh"))
    return finish(arrived, tokens, n_y)


def solution(mesh):
    finer = Mesh(mesh.devices.reshape(2, 4, 8, 2, 2), ALL)
    return jax.shard_map(
        block,
        mesh=finer,
        in_specs=(
            P(ALL, None),
            P(),
            P(DP, MP),
            P(DP, MP),
            P(DP, MP),
            P(DP, MP),
            P(MP),
            P(MP, DP),
            P(MP, DP),
            P(MP),
        ),
        out_specs=P(ALL, None),
        check_vma=False,
    )
```

```python
import functools
import math

import jax
import jax.numpy as jnp
from jax import lax
from jax.experimental import pallas as pl
from jax.experimental.pallas import tpu as pltpu
from jax.sharding import Mesh
from jax.sharding import PartitionSpec as P


HEAD = 128
DP = ("xl", "y")
MP = ("z", "xh", "c")
ALL = DP + MP
BF = jnp.bfloat16
F32 = jnp.float32
ANY = pl.BlockSpec(memory_space=pl.ANY)
VMEM = pl.BlockSpec(memory_space=pltpu.VMEM)


def normalize(values):
    center = values - jnp.mean(values, axis=-1, keepdims=True)
    spread = jnp.mean(center * center, axis=-1, keepdims=True)
    return center * lax.rsqrt(spread + 1e-06)


def partner(array, axis):
    return lax.ppermute(array, axis, [(0, 1), (1, 0)])


def exchange(pieces, axes):
    return lax.all_to_all(pieces, axes, split_axis=0, concat_axis=0, tiled=True)


def dot(a, b):
    return lax.dot_general(a, b, (((a.ndim - 1,), (0,)), ((), ())), preferred_element_type=F32)


def params(mib):
    return pltpu.CompilerParams(vmem_limit_bytes=mib * 1024 * 1024)


def cost(flops, moved):
    return pl.CostEstimate(flops=flops, bytes_accessed=moved, transcendentals=0)


def norm_kernel(tokens, norm_gain, normed, gain, own, sems):
    copies = [
        pltpu.make_async_copy(tokens, own, sems.at[0]),
        pltpu.make_async_copy(norm_gain, gain, sems.at[1]),
    ]
    for copy in copies:
        copy.start()
    copies[0].wait()
    values = normalize(own[...].astype(F32))
    copies[1].wait()
    normed[...] = values * gain[...]


def norm_own(tokens, gain):
    count, width = tokens.shape
    return pl.pallas_call(
        norm_kernel,
        out_shape=(
            jax.ShapeDtypeStruct((count, width), F32),
            jax.ShapeDtypeStruct((1, width), F32),
        ),
        in_specs=[ANY] * 2,
        out_specs=(VMEM, VMEM),
        scratch_shapes=[pltpu.VMEM((count, width), BF), pltpu.SemaphoreType.DMA((2,))],
        compiler_params=params(8),
        cost_estimate=cost(100 * count * width, 1024 * 1024),
        name="norm_own",
    )(tokens, gain.reshape(1, width))


def spread_kernel(n_y, n_z, normed_own, gain, beside, out):
    _, width = beside.shape
    cols = width // (2 * n_y)
    mine = normed_own[...]
    theirs = normalize(beside[...].astype(F32)) * gain[...]
    first = lax.axis_index("xh") == 0
    normed = jnp.concatenate(
        (jnp.where(first, mine, theirs), jnp.where(first, theirs, mine)), axis=0
    )
    lower = lax.axis_index("xl") == 0
    for y in range(n_y):
        a = normed[:, y * cols : (y + 1) * cols]
        b = normed[:, (n_y + y) * cols : (n_y + y + 1) * cols]
        left = jnp.where(lower, a, b).astype(BF)
        right = jnp.where(lower, b, a).astype(BF)
        for z in range(n_z):
            out[z * n_y + y, :, :cols] = left
            out[z * n_y + y, :, cols:] = right


def spread(normed_own, gain, beside, n_y, n_z):
    count, width = beside.shape
    return pl.pallas_call(
        functools.partial(spread_kernel, n_y, n_z),
        out_shape=jax.ShapeDtypeStruct((n_z * n_y, 2 * count, width // n_y), BF),
        in_specs=[VMEM] * 3,
        out_specs=VMEM,
        compiler_params=params(8),
        cost_estimate=cost(20 * count * width, 2 * 1024 * 1024),
        name="normed_pieces",
    )(normed_own, gain, beside)


def product(rows, w, w_p, at):
    cols = rows.shape[1] // 2
    return dot(rows[:, :cols], w[:, at]) + dot(rows[:, cols:], w_p[:, at])


def store(out, value, first, at):
    n_y = out.shape[0]
    value = value.astype(BF).reshape(-1, n_y, 8, value.shape[-1])
    for y in range(n_y):
        part = value[:, y].reshape(-1, value.shape[-1])
        out[y, first : first + part.shape[0], at] = part


def inner_kernel(tokens, w_own, w_other, out, rows, kept, kept_p, sems):
    chunk = 384
    first = pltpu.make_async_copy(tokens, rows, sems.at[0])
    copies = []
    for n in range(kept.shape[1] // chunk):
        at = pl.ds(n * chunk, chunk)
        for m, (source, to) in enumerate(((w_own, kept), (w_other, kept_p))):
            copies.append(
                pltpu.make_async_copy(source.at[:, at], to.at[:, at], sems.at[1 + 2 * n + m])
            )
    copies[0].start()
    first.start()
    for copy in copies[1:]:
        copy.start()
    first.wait()
    left = rows[...].reshape(-1, rows.shape[-1])
    for n in range(kept.shape[1] // chunk):
        copies[2 * n].wait()
        copies[2 * n + 1].wait()
        at = slice(n * chunk, (n + 1) * chunk)
        store(out, product(left, kept, kept_p, at), 0, at)


def inner_part(tokens, w_own, w_other, images):
    pieces, count, width = tokens.shape
    half = pieces * count // images
    columns = w_own.shape[1]
    return pl.pallas_call(
        inner_kernel,
        out_shape=jax.ShapeDtypeStruct((images, half, columns), BF),
        in_specs=[ANY, ANY, ANY],
        out_specs=VMEM,
        scratch_shapes=[
            pltpu.VMEM(tokens.shape, BF),
            pltpu.VMEM(w_own.shape, BF),
            pltpu.VMEM(w_other.shape, BF),
            pltpu.SemaphoreType.DMA((5,)),
        ],
        compiler_params=params(12),
        cost_estimate=cost(2 * images * half * width * columns, 4 * 1024 * 1024),
        name="inner_part",
    )(tokens, w_own, w_other)


def heads_kernel(
    mine, theirs, w_own, w_other, inner_mine, inner_theirs, out, rows, rows_p, kept, kept_p, sems
):
    width, wide = rows.shape[-1], w_own.shape[1]
    half = out.shape[1] // 2
    copies = [
        pltpu.make_async_copy(mine, rows, sems.at[0]),
        pltpu.make_async_copy(w_own, kept, sems.at[1]),
        pltpu.make_async_copy(w_other, kept_p, sems.at[2]),
        pltpu.make_async_copy(theirs, rows_p, sems.at[3]),
        pltpu.make_async_copy(inner_mine, out.at[:, :half, wide:], sems.at[4]),
        pltpu.make_async_copy(inner_theirs, out.at[:, half:, wide:], sems.at[5]),
    ]
    for copy in copies:
        copy.start()
    cols = width // 2
    copies[0].wait()
    copies[1].wait()
    left = rows[...].reshape(-1, width)
    own = dot(left[:, :cols], kept[...])
    copies[2].wait()
    store(out, own + dot(left[:, cols:], kept_p[...]), 0, slice(0, wide))
    copies[3].wait()
    left = rows_p[...].reshape(-1, width)
    value = dot(left[:, :cols], kept[...]) + dot(left[:, cols:], kept_p[...])
    store(out, value, half, slice(0, wide))
    for copy in copies[4:]:
        copy.wait()


def heads_part(mine, theirs, w_own, w_other, inner_mine, inner_theirs):
    images, half, _ = inner_mine.shape
    width, wide = mine.shape[-1], w_own.shape[1]
    return pl.pallas_call(
        heads_kernel,
        out_shape=jax.ShapeDtypeStruct((images, 2 * half, wide + inner_mine.shape[2]), BF),
        in_specs=[ANY, ANY, ANY, ANY, ANY, ANY],
        out_specs=VMEM,
        scratch_shapes=[pltpu.VMEM(mine.shape, BF)] * 2
        + [pltpu.VMEM(w_own.shape, BF)] * 2
        + [pltpu.SemaphoreType.DMA((6,))],
        compiler_params=params(12),
        cost_estimate=cost(4 * images * half * width * wide, 4 * 1024 * 1024),
        name="heads_part",
    )(mine, theirs, w_own, w_other, inner_mine, inner_theirs)


def middle_kernel(arrived, bias, scale, out, kept, sem):
    copy = pltpu.make_async_copy(bias, kept, sem)
    copy.start()
    copies, columns = out.shape[0], kept.shape[0]

    def summed(at):
        total = arrived[0, :, at].astype(F32)
        for n in range(1, arrived.shape[0]):
            total = total + arrived[n, :, at].astype(F32)
        return total

    def rounded(n):
        return summed(slice(n * HEAD, (n + 1) * HEAD)).astype(BF)

    query_norm = normalize(rounded(0).astype(F32)).astype(BF)
    key_norm = normalize(rounded(1).astype(F32)).astype(BF)
    scores = lax.dot_general(
        query_norm, key_norm, (((1,), (1,)), ((), ())), preferred_element_type=F32
    )
    scores = scores * scale[0]
    powers = jnp.exp(scores - jnp.max(scores, axis=-1, keepdims=True))
    probs = (powers / jnp.sum(powers, axis=-1, keepdims=True)).astype(BF)
    mixed = dot(probs, rounded(2)).astype(BF)
    for n in range(copies):
        out[n, :, :HEAD] = mixed
    copy.wait()
    for m in range(columns // 256):
        at = slice(m * 256, (m + 1) * 256)
        inner = summed(slice(3 * HEAD + m * 256, 3 * HEAD + (m + 1) * 256)) + kept[at]
        activ = (inner * (0.5 + 0.5 * lax.erf(inner * math.sqrt(0.5)))).astype(BF)
        for n in range(copies):
            out[n, :, HEAD + m * 256 : HEAD + (m + 1) * 256] = activ


def middle(arrived, bias, scale):
    _, patches, _ = arrived.shape
    columns = bias.shape[0]
    return pl.pallas_call(
        middle_kernel,
        out_shape=jax.ShapeDtypeStruct((1, patches, HEAD + columns), BF),
        in_specs=[VMEM, ANY, pl.BlockSpec(memory_space=pltpu.SMEM)],
        out_specs=VMEM,
        scratch_shapes=[pltpu.VMEM((columns,), F32), pltpu.SemaphoreType.DMA],
        compiler_params=params(12),
        cost_estimate=cost(60 * patches * columns, 2 * 1024 * 1024),
        name="middle",
    )(arrived, bias, scale)


def output_kernel(part, features, w_own, w_other, out, rows, kept_own, kept_other, sems):
    images, half, width = rows.shape
    cols = kept_own.shape[1]
    copies = [
        pltpu.make_async_copy(
            features.at[:, part * half : (part + 1) * half], rows, sems.at[0]
        ),
        pltpu.make_async_copy(w_own, kept_own, sems.at[1]),
        pltpu.make_async_copy(w_other, kept_other, sems.at[2]),
    ]
    for copy in copies:
        copy.start()
    copies[0].wait()
    left = rows[...].reshape(images * half, width)
    for n, kept in enumerate((kept_own, kept_other)):
        copies[n + 1].wait()
        for m in range(2):
            at = slice(m * cols // 2, (m + 1) * cols // 2)
            value = dot(left, kept[:, at]).astype(out.dtype).reshape(images, half, cols // 2)
            out[:, :, n * cols + m * cols // 2 : n * cols + (m + 1) * cols // 2] = value


def output(features, w_own, w_other, part, kind):
    images, patches, width = features.shape
    half, cols = patches // 2, w_own.shape[1]
    return pl.pallas_call(
        functools.partial(output_kernel, part),
        out_shape=jax.ShapeDtypeStruct((images, half, 2 * cols), kind),
        in_specs=[ANY] * 3,
        out_specs=VMEM,
        scratch_shapes=[
            pltpu.VMEM((images, half, width), BF),
            pltpu.VMEM(w_own.shape, BF),
            pltpu.VMEM(w_other.shape, BF),
            pltpu.SemaphoreType.DMA((3,)),
        ],
        compiler_params=params(16),
        cost_estimate=cost(4 * images * half * width * cols, 4 * 1024 * 1024),
        name="output_sent" if part else "output_kept",
    )(features, w_own, w_other)


def combine_kernel(n_xh, kept, received, out):
    images, half, _ = kept.shape
    n_z = half // 8
    count = 8 // n_xh
    for y in range(images):
        for z in range(n_z):
            at = slice(z * 8, (z + 1) * 8)
            value = kept[y, at] + received[y, at].astype(F32)
            for xh in range(n_xh):
                out[(xh * n_z + z) * images + y] = value[xh * count : (xh + 1) * count].astype(BF)


def combine(kept, received, n_xh):
    images, half, width = kept.shape
    count = 8 // n_xh
    return pl.pallas_call(
        functools.partial(combine_kernel, n_xh),
        out_shape=jax.ShapeDtypeStruct((images * half // count, count, width), BF),
        in_specs=[VMEM] * 2,
        out_specs=VMEM,
        compiler_params=params(8),
        cost_estimate=cost(kept.size, 4 * 1024 * 1024),
        name="combine",
    )(kept, received)


def finish_kernel(n_y, arrived, tokens, out):
    pieces, _, width = arrived.shape
    cols = width // 2
    lower = lax.axis_index("xl") == 0
    for y in range(n_y):
        total = arrived[y].astype(F32)
        for n in range(y + n_y, pieces, n_y):
            total = total + arrived[n].astype(F32)
        left, right = total[:, :cols], total[:, cols:]
        for n, value in enumerate(
            (jnp.where(lower, left, right), jnp.where(lower, right, left))
        ):
            to = slice((n * n_y + y) * cols, (n * n_y + y + 1) * cols)
            out[:, to] = (tokens[:, to].astype(F32) + value).astype(BF)


def finish(arrived, tokens, n_y):
    return pl.pallas_call(
        functools.partial(finish_kernel, n_y),
        out_shape=jax.ShapeDtypeStruct(tokens.shape, BF),
        in_specs=[VMEM] * 2,
        out_specs=VMEM,
        compiler_params=params(8),
        cost_estimate=cost(arrived.size, 2 * 1024 * 1024),
        name="finish",
    )(arrived, tokens)


def block(
    tokens, norm_gain, w_query, w_key, w_value, w_inner, bias_inner, w_attn_out, w_outer, temper
):
    n_y, n_z, n_xh = (lax.axis_size(a) for a in ("y", "z", "xh"))
    beside = partner(tokens, "xh")
    w_qkv = jnp.concatenate((w_query, w_key, w_value), axis=1)
    w_inner_p = partner(w_inner, "xl")
    w_qkv_p = partner(w_qkv, "xl")
    w_out = jnp.concatenate((w_attn_out, w_outer), axis=0)
    w_out_p = partner(w_out, "xl")
    normed, gain = norm_own(tokens, norm_gain)
    pieces = spread(normed, gain, beside, n_y, n_z)
    mine = exchange(pieces, ("z", "y"))
    theirs = partner(mine, "c")
    inner_mine = inner_part(mine, w_inner, w_inner_p, n_y)
    inner_theirs = inner_part(theirs, w_inner, w_inner_p, n_y)
    partial = heads_part(mine, theirs, w_qkv, w_qkv_p, inner_mine, inner_theirs)
    arrived = exchange(partial, "y")
    scale = temper / math.sqrt(HEAD)
    features = middle(arrived, bias_inner, scale)[0]
    features = lax.all_gather(features, "y", axis=0, tiled=False)
    sent = partner(output(features, w_out, w_out_p, 1, BF), "c")
    kept = output(features, w_out, w_out_p, 0, F32)
    pieces = combine(kept, sent, n_xh)
    arrived = exchange(pieces, ("xh", "z", "y"))
    return finish(arrived, tokens, n_y)


def solution(mesh):
    finer = Mesh(mesh.devices.reshape(2, 4, 8, 2, 2), ALL)
    return jax.shard_map(
        block,
        mesh=finer,
        in_specs=(
            P(ALL, None),
            P(),
            P(DP, MP),
            P(DP, MP),
            P(DP, MP),
            P(DP, MP),
            P(MP),
            P(MP, DP),
            P(MP, DP),
            P(MP),
        ),
        out_specs=P(ALL, None),
        check_vma=False,
    )
```

```python
import functools
import math

import jax
import jax.numpy as jnp
from jax import lax
from jax.experimental import pallas as pl
from jax.experimental.pallas import tpu as pltpu
from jax.sharding import Mesh
from jax.sharding import PartitionSpec as P


HEAD = 128
DP = ("xl", "y")
MP = ("z", "xh", "c")
ALL = DP + MP
BF = jnp.bfloat16
F32 = jnp.float32
ANY = pl.BlockSpec(memory_space=pl.ANY)
VMEM = pl.BlockSpec(memory_space=pltpu.VMEM)


def normalize(values):
    center = values - jnp.mean(values, axis=-1, keepdims=True)
    spread = jnp.mean(center * center, axis=-1, keepdims=True)
    return center * lax.rsqrt(spread + 1e-06)


def partner(array, axis):
    return lax.ppermute(array, axis, [(0, 1), (1, 0)])


def exchange(pieces, axes):
    return lax.all_to_all(pieces, axes, split_axis=0, concat_axis=0, tiled=True)


def dot(a, b):
    return lax.dot_general(a, b, (((a.ndim - 1,), (0,)), ((), ())), preferred_element_type=F32)


def params(mib):
    return pltpu.CompilerParams(vmem_limit_bytes=mib * 1024 * 1024)


def cost(flops, moved):
    return pl.CostEstimate(flops=flops, bytes_accessed=moved, transcendentals=0)


def norm_kernel(tokens, norm_gain, normed, gain, own, sems):
    copies = [
        pltpu.make_async_copy(tokens, own, sems.at[0]),
        pltpu.make_async_copy(norm_gain, gain, sems.at[1]),
    ]
    for copy in copies:
        copy.start()
    copies[0].wait()
    values = normalize(own[...].astype(F32))
    copies[1].wait()
    normed[...] = values * gain[...]


def norm_own(tokens, gain):
    count, width = tokens.shape
    return pl.pallas_call(
        norm_kernel,
        out_shape=(
            jax.ShapeDtypeStruct((count, width), F32),
            jax.ShapeDtypeStruct((1, width), F32),
        ),
        in_specs=[ANY] * 2,
        out_specs=(VMEM, VMEM),
        scratch_shapes=[pltpu.VMEM((count, width), BF), pltpu.SemaphoreType.DMA((2,))],
        compiler_params=params(8),
        cost_estimate=cost(100 * count * width, 1024 * 1024),
        name="norm_own",
    )(tokens, gain.reshape(1, width))


def spread_kernel(n_y, n_z, normed_own, gain, beside, out):
    _, width = beside.shape
    cols = width // (2 * n_y)
    mine = normed_own[...]
    theirs = normalize(beside[...].astype(F32)) * gain[...]
    first = lax.axis_index("xh") == 0
    normed = jnp.concatenate(
        (jnp.where(first, mine, theirs), jnp.where(first, theirs, mine)), axis=0
    )
    lower = lax.axis_index("xl") == 0
    for y in range(n_y):
        a = normed[:, y * cols : (y + 1) * cols]
        b = normed[:, (n_y + y) * cols : (n_y + y + 1) * cols]
        left = jnp.where(lower, a, b).astype(BF)
        right = jnp.where(lower, b, a).astype(BF)
        for z in range(n_z):
            out[z * n_y + y, :, :cols] = left
            out[z * n_y + y, :, cols:] = right


def spread(normed_own, gain, beside, n_y, n_z):
    count, width = beside.shape
    return pl.pallas_call(
        functools.partial(spread_kernel, n_y, n_z),
        out_shape=jax.ShapeDtypeStruct((n_z * n_y, 2 * count, width // n_y), BF),
        in_specs=[VMEM] * 3,
        out_specs=VMEM,
        compiler_params=params(8),
        cost_estimate=cost(20 * count * width, 2 * 1024 * 1024),
        name="normed_pieces",
    )(normed_own, gain, beside)


def product(rows, w, w_p, at):
    cols = rows.shape[1] // 2
    return dot(rows[:, :cols], w[:, at]) + dot(rows[:, cols:], w_p[:, at])


def store(out, value, first, at):
    n_y = out.shape[0]
    value = value.astype(BF).reshape(-1, n_y, 8, value.shape[-1])
    for y in range(n_y):
        part = value[:, y].reshape(-1, value.shape[-1])
        out[y, first : first + part.shape[0], at] = part


def inner_kernel(rows, w_own, w_other, out, kept_p, sems):
    chunk = 384
    chunks = w_own.shape[1] // chunk
    copies = []
    for n in range(chunks):
        at = pl.ds(n * chunk, chunk)
        copies.append(pltpu.make_async_copy(w_other.at[:, at], kept_p.at[:, at], sems.at[n]))
    for copy in copies:
        copy.start()
    left = rows[...].reshape(-1, rows.shape[-1])
    for n in range(chunks):
        copies[n].wait()
        at = slice(n * chunk, (n + 1) * chunk)
        store(out, product(left, w_own, kept_p, at), 0, at)


def inner_part(tokens, w_own, w_other, images):
    pieces, count, width = tokens.shape
    half = pieces * count // images
    columns = w_own.shape[1]
    return pl.pallas_call(
        inner_kernel,
        out_shape=jax.ShapeDtypeStruct((images, half, columns), BF),
        in_specs=[VMEM, VMEM, ANY],
        out_specs=VMEM,
        scratch_shapes=[pltpu.VMEM(w_other.shape, BF), pltpu.SemaphoreType.DMA((2,))],
        compiler_params=params(12),
        cost_estimate=cost(2 * images * half * width * columns, 4 * 1024 * 1024),
        name="inner_part",
    )(tokens, w_own, w_other)


def heads_kernel(
    mine, theirs, w_own, w_other, inner_mine, inner_theirs, out, kept, kept_p, sems
):
    width, wide = mine.shape[-1], w_own.shape[1]
    half = out.shape[1] // 2
    copies = [
        pltpu.make_async_copy(w_own, kept, sems.at[0]),
        pltpu.make_async_copy(w_other, kept_p, sems.at[1]),
        pltpu.make_async_copy(inner_mine, out.at[:, :half, wide:], sems.at[2]),
        pltpu.make_async_copy(inner_theirs, out.at[:, half:, wide:], sems.at[3]),
    ]
    for copy in copies:
        copy.start()
    cols = width // 2
    copies[0].wait()
    left = mine[...].reshape(-1, width)
    own = dot(left[:, :cols], kept[...])
    copies[1].wait()
    store(out, own + dot(left[:, cols:], kept_p[...]), 0, slice(0, wide))
    left = theirs[...].reshape(-1, width)
    value = dot(left[:, :cols], kept[...]) + dot(left[:, cols:], kept_p[...])
    store(out, value, half, slice(0, wide))
    for copy in copies[2:]:
        copy.wait()


def heads_part(mine, theirs, w_own, w_other, inner_mine, inner_theirs):
    images, half, _ = inner_mine.shape
    width, wide = mine.shape[-1], w_own.shape[1]
    return pl.pallas_call(
        heads_kernel,
        out_shape=jax.ShapeDtypeStruct((images, 2 * half, wide + inner_mine.shape[2]), BF),
        in_specs=[VMEM, VMEM, ANY, ANY, ANY, ANY],
        out_specs=VMEM,
        scratch_shapes=[pltpu.VMEM(w_own.shape, BF)] * 2 + [pltpu.SemaphoreType.DMA((4,))],
        compiler_params=params(12),
        cost_estimate=cost(4 * images * half * width * wide, 4 * 1024 * 1024),
        name="heads_part",
    )(mine, theirs, w_own, w_other, inner_mine, inner_theirs)


def middle_kernel(arrived, bias, scale, out, kept, sem):
    copy = pltpu.make_async_copy(bias, kept, sem)
    copy.start()
    copies, columns = out.shape[0], kept.shape[0]

    def summed(at):
        total = arrived[0, :, at].astype(F32)
        for n in range(1, arrived.shape[0]):
            total = total + arrived[n, :, at].astype(F32)
        return total

    def rounded(n):
        return summed(slice(n * HEAD, (n + 1) * HEAD)).astype(BF)

    query_norm = normalize(rounded(0).astype(F32)).astype(BF)
    key_norm = normalize(rounded(1).astype(F32)).astype(BF)
    scores = lax.dot_general(
        query_norm, key_norm, (((1,), (1,)), ((), ())), preferred_element_type=F32
    )
    scores = scores * scale[0]
    powers = jnp.exp(scores - jnp.max(scores, axis=-1, keepdims=True))
    probs = (powers / jnp.sum(powers, axis=-1, keepdims=True)).astype(BF)
    mixed = dot(probs, rounded(2)).astype(BF)
    for n in range(copies):
        out[n, :, :HEAD] = mixed
    copy.wait()
    for m in range(columns // 256):
        at = slice(m * 256, (m + 1) * 256)
        inner = summed(slice(3 * HEAD + m * 256, 3 * HEAD + (m + 1) * 256)) + kept[at]
        activ = (inner * (0.5 + 0.5 * lax.erf(inner * math.sqrt(0.5)))).astype(BF)
        for n in range(copies):
            out[n, :, HEAD + m * 256 : HEAD + (m + 1) * 256] = activ


def middle(arrived, bias, scale):
    _, patches, _ = arrived.shape
    columns = bias.shape[0]
    return pl.pallas_call(
        middle_kernel,
        out_shape=jax.ShapeDtypeStruct((1, patches, HEAD + columns), BF),
        in_specs=[VMEM, ANY, pl.BlockSpec(memory_space=pltpu.SMEM)],
        out_specs=VMEM,
        scratch_shapes=[pltpu.VMEM((columns,), F32), pltpu.SemaphoreType.DMA],
        compiler_params=params(12),
        cost_estimate=cost(60 * patches * columns, 2 * 1024 * 1024),
        name="middle",
    )(arrived, bias, scale)


def output_kernel(part, features, w_own, w_other, out):
    images, half, _ = out.shape
    cols = w_own.shape[1]
    left = features[:, part * half : (part + 1) * half].reshape(images * half, -1)
    for n, weights in enumerate((w_own, w_other)):
        for m in range(2):
            at = slice(m * cols // 2, (m + 1) * cols // 2)
            value = dot(left, weights[:, at]).astype(out.dtype)
            to = slice(n * cols + m * cols // 2, n * cols + (m + 1) * cols // 2)
            out[:, :, to] = value.reshape(images, half, cols // 2)


def output(features, w_own, w_other, part, kind):
    images, patches, width = features.shape
    half, cols = patches // 2, w_own.shape[1]
    return pl.pallas_call(
        functools.partial(output_kernel, part),
        out_shape=jax.ShapeDtypeStruct((images, half, 2 * cols), kind),
        in_specs=[VMEM] * 3,
        out_specs=VMEM,
        compiler_params=params(16),
        cost_estimate=cost(4 * images * half * width * cols, 4 * 1024 * 1024),
        name="output_sent" if part else "output_kept",
    )(features, w_own, w_other)


def combine_kernel(n_xh, kept, received, out):
    images, half, _ = kept.shape
    n_z = half // 8
    count = 8 // n_xh
    for y in range(images):
        for z in range(n_z):
            at = slice(z * 8, (z + 1) * 8)
            value = kept[y, at] + received[y, at].astype(F32)
            for xh in range(n_xh):
                out[(xh * n_z + z) * images + y] = value[xh * count : (xh + 1) * count].astype(BF)


def combine(kept, received, n_xh):
    images, half, width = kept.shape
    count = 8 // n_xh
    return pl.pallas_call(
        functools.partial(combine_kernel, n_xh),
        out_shape=jax.ShapeDtypeStruct((images * half // count, count, width), BF),
        in_specs=[VMEM] * 2,
        out_specs=VMEM,
        compiler_params=params(8),
        cost_estimate=cost(kept.size, 4 * 1024 * 1024),
        name="combine",
    )(kept, received)


def finish_kernel(n_y, arrived, tokens, out):
    pieces, _, width = arrived.shape
    cols = width // 2
    lower = lax.axis_index("xl") == 0
    for y in range(n_y):
        total = arrived[y].astype(F32)
        for n in range(y + n_y, pieces, n_y):
            total = total + arrived[n].astype(F32)
        left, right = total[:, :cols], total[:, cols:]
        for n, value in enumerate(
            (jnp.where(lower, left, right), jnp.where(lower, right, left))
        ):
            to = slice((n * n_y + y) * cols, (n * n_y + y + 1) * cols)
            out[:, to] = (tokens[:, to].astype(F32) + value).astype(BF)


def finish(arrived, tokens, n_y):
    return pl.pallas_call(
        functools.partial(finish_kernel, n_y),
        out_shape=jax.ShapeDtypeStruct(tokens.shape, BF),
        in_specs=[VMEM] * 2,
        out_specs=VMEM,
        compiler_params=params(8),
        cost_estimate=cost(arrived.size, 2 * 1024 * 1024),
        name="finish",
    )(arrived, tokens)


def block(
    tokens, norm_gain, w_query, w_key, w_value, w_inner, bias_inner, w_attn_out, w_outer, temper
):
    n_y, n_z, n_xh = (lax.axis_size(a) for a in ("y", "z", "xh"))
    beside = partner(tokens, "xh")
    w_qkv = jnp.concatenate((w_query, w_key, w_value), axis=1)
    w_inner_p = partner(w_inner, "xl")
    w_qkv_p = partner(w_qkv, "xl")
    w_out = jnp.concatenate((w_attn_out, w_outer), axis=0)
    w_out_p = partner(w_out, "xl")
    normed, gain = norm_own(tokens, norm_gain)
    pieces = spread(normed, gain, beside, n_y, n_z)
    mine = exchange(pieces, ("z", "y"))
    theirs = partner(mine, "c")
    inner_mine = inner_part(mine, w_inner, w_inner_p, n_y)
    inner_theirs = inner_part(theirs, w_inner, w_inner_p, n_y)
    partial = heads_part(mine, theirs, w_qkv, w_qkv_p, inner_mine, inner_theirs)
    arrived = exchange(partial, "y")
    scale = temper / math.sqrt(HEAD)
    features = middle(arrived, bias_inner, scale)[0]
    features = lax.all_gather(features, "y", axis=0, tiled=False)
    sent = partner(output(features, w_out, w_out_p, 1, BF), "c")
    kept = output(features, w_out, w_out_p, 0, F32)
    pieces = combine(kept, sent, n_xh)
    arrived = exchange(pieces, ("xh", "z", "y"))
    return finish(arrived, tokens, n_y)


def solution(mesh):
    finer = Mesh(mesh.devices.reshape(2, 4, 8, 2, 2), ALL)
    return jax.shard_map(
        block,
        mesh=finer,
        in_specs=(
            P(ALL, None),
            P(),
            P(DP, MP),
            P(DP, MP),
            P(DP, MP),
            P(DP, MP),
            P(MP),
            P(MP, DP),
            P(MP, DP),
            P(MP),
        ),
        out_specs=P(ALL, None),
        check_vma=False,
    )
```

```python
import functools
import math

import jax
import jax.numpy as jnp
from jax import lax
from jax.experimental import pallas as pl
from jax.experimental.pallas import tpu as pltpu
from jax.sharding import Mesh
from jax.sharding import PartitionSpec as P


HEAD = 128
DP = ("xl", "y")
MP = ("z", "xh", "c")
ALL = DP + MP
BF = jnp.bfloat16
F32 = jnp.float32
ANY = pl.BlockSpec(memory_space=pl.ANY)
VMEM = pl.BlockSpec(memory_space=pltpu.VMEM)


def normalize(values):
    center = values - jnp.mean(values, axis=-1, keepdims=True)
    spread = jnp.mean(center * center, axis=-1, keepdims=True)
    return center * lax.rsqrt(spread + 1e-06)


def partner(array, axis):
    return lax.ppermute(array, axis, [(0, 1), (1, 0)])


def exchange(pieces, axes):
    return lax.all_to_all(pieces, axes, split_axis=0, concat_axis=0, tiled=True)


def dot(a, b):
    return lax.dot_general(a, b, (((a.ndim - 1,), (0,)), ((), ())), preferred_element_type=F32)


def params(mib):
    return pltpu.CompilerParams(vmem_limit_bytes=mib * 1024 * 1024)


def cost(flops, moved):
    return pl.CostEstimate(flops=flops, bytes_accessed=moved, transcendentals=0)


def norm_kernel(tokens, norm_gain, normed, gain, own, sems):
    copies = [
        pltpu.make_async_copy(tokens, own, sems.at[0]),
        pltpu.make_async_copy(norm_gain, gain, sems.at[1]),
    ]
    for copy in copies:
        copy.start()
    copies[0].wait()
    values = normalize(own[...].astype(F32))
    copies[1].wait()
    normed[...] = values * gain[...]


def norm_own(tokens, gain):
    count, width = tokens.shape
    return pl.pallas_call(
        norm_kernel,
        out_shape=(
            jax.ShapeDtypeStruct((count, width), F32),
            jax.ShapeDtypeStruct((1, width), F32),
        ),
        in_specs=[ANY] * 2,
        out_specs=(VMEM, VMEM),
        scratch_shapes=[pltpu.VMEM((count, width), BF), pltpu.SemaphoreType.DMA((2,))],
        compiler_params=params(8),
        cost_estimate=cost(100 * count * width, 1024 * 1024),
        name="norm_own",
    )(tokens, gain.reshape(1, width))


def spread_kernel(n_y, n_z, normed_own, gain, beside, out):
    _, width = beside.shape
    cols = width // (2 * n_y)
    mine = normed_own[...]
    theirs = normalize(beside[...].astype(F32)) * gain[...]
    first = lax.axis_index("xh") == 0
    normed = jnp.concatenate(
        (jnp.where(first, mine, theirs), jnp.where(first, theirs, mine)), axis=0
    )
    lower = lax.axis_index("xl") == 0
    for y in range(n_y):
        a = normed[:, y * cols : (y + 1) * cols]
        b = normed[:, (n_y + y) * cols : (n_y + y + 1) * cols]
        left = jnp.where(lower, a, b).astype(BF)
        right = jnp.where(lower, b, a).astype(BF)
        for z in range(n_z):
            out[z * n_y + y, :, :cols] = left
            out[z * n_y + y, :, cols:] = right


def spread(normed_own, gain, beside, n_y, n_z):
    count, width = beside.shape
    return pl.pallas_call(
        functools.partial(spread_kernel, n_y, n_z),
        out_shape=jax.ShapeDtypeStruct((n_z * n_y, 2 * count, width // n_y), BF),
        in_specs=[VMEM] * 3,
        out_specs=VMEM,
        compiler_params=params(8),
        cost_estimate=cost(20 * count * width, 2 * 1024 * 1024),
        name="normed_pieces",
    )(normed_own, gain, beside)


def product(rows, w, w_p, at):
    cols = rows.shape[1] // 2
    return dot(rows[:, :cols], w[:, at]) + dot(rows[:, cols:], w_p[:, at])


def store(out, value, first, at):
    n_y = out.shape[0]
    value = value.astype(BF).reshape(-1, n_y, 8, value.shape[-1])
    for y in range(n_y):
        part = value[:, y].reshape(-1, value.shape[-1])
        out[y, first : first + part.shape[0], at] = part


def inner_kernel(rows, w_own, w_other, out, kept_p, sems):
    chunk = 384
    chunks = w_own.shape[1] // chunk
    copies = []
    for n in range(chunks):
        at = pl.ds(n * chunk, chunk)
        copies.append(pltpu.make_async_copy(w_other.at[:, at], kept_p.at[:, at], sems.at[n]))
    for copy in copies:
        copy.start()
    left = rows[...].reshape(-1, rows.shape[-1])
    for n in range(chunks):
        copies[n].wait()
        at = slice(n * chunk, (n + 1) * chunk)
        store(out, product(left, w_own, kept_p, at), 0, at)


def inner_part(tokens, w_own, w_other, images):
    pieces, count, width = tokens.shape
    half = pieces * count // images
    columns = w_own.shape[1]
    return pl.pallas_call(
        inner_kernel,
        out_shape=jax.ShapeDtypeStruct((images, half, columns), BF),
        in_specs=[VMEM, VMEM, ANY],
        out_specs=VMEM,
        scratch_shapes=[pltpu.VMEM(w_other.shape, BF), pltpu.SemaphoreType.DMA((2,))],
        compiler_params=params(12),
        cost_estimate=cost(2 * images * half * width * columns, 4 * 1024 * 1024),
        name="inner_part",
    )(tokens, w_own, w_other)


def heads_kernel(
    mine, theirs, w_own, w_other, inner_mine, inner_theirs, out, kept, kept_p, sems
):
    width, wide = mine.shape[-1], w_own.shape[1]
    half = out.shape[1] // 2
    copies = [
        pltpu.make_async_copy(w_own, kept, sems.at[0]),
        pltpu.make_async_copy(w_other, kept_p, sems.at[1]),
        pltpu.make_async_copy(inner_mine, out.at[:, :half, wide:], sems.at[2]),
        pltpu.make_async_copy(inner_theirs, out.at[:, half:, wide:], sems.at[3]),
    ]
    for copy in copies:
        copy.start()
    cols = width // 2
    copies[0].wait()
    left = mine[...].reshape(-1, width)
    own = dot(left[:, :cols], kept[...])
    copies[1].wait()
    store(out, own + dot(left[:, cols:], kept_p[...]), 0, slice(0, wide))
    left = theirs[...].reshape(-1, width)
    value = dot(left[:, :cols], kept[...]) + dot(left[:, cols:], kept_p[...])
    store(out, value, half, slice(0, wide))
    for copy in copies[2:]:
        copy.wait()


def heads_part(mine, theirs, w_own, w_other, inner_mine, inner_theirs):
    images, half, _ = inner_mine.shape
    width, wide = mine.shape[-1], w_own.shape[1]
    return pl.pallas_call(
        heads_kernel,
        out_shape=jax.ShapeDtypeStruct((images, 2 * half, wide + inner_mine.shape[2]), BF),
        in_specs=[VMEM, VMEM, ANY, ANY, ANY, ANY],
        out_specs=VMEM,
        scratch_shapes=[pltpu.VMEM(w_own.shape, BF)] * 2 + [pltpu.SemaphoreType.DMA((4,))],
        compiler_params=params(12),
        cost_estimate=cost(4 * images * half * width * wide, 4 * 1024 * 1024),
        name="heads_part",
    )(mine, theirs, w_own, w_other, inner_mine, inner_theirs)


def middle_kernel(arrived, bias, scale, out, kept, sem):
    copy = pltpu.make_async_copy(bias, kept, sem)
    copy.start()
    copies, columns = out.shape[0], kept.shape[0]

    def summed(at):
        total = arrived[0, :, at].astype(F32)
        for n in range(1, arrived.shape[0]):
            total = total + arrived[n, :, at].astype(F32)
        return total

    def rounded(n):
        return summed(slice(n * HEAD, (n + 1) * HEAD)).astype(BF)

    query_norm = normalize(rounded(0).astype(F32)).astype(BF)
    key_norm = normalize(rounded(1).astype(F32)).astype(BF)
    scores = lax.dot_general(
        query_norm, key_norm, (((1,), (1,)), ((), ())), preferred_element_type=F32
    )
    scores = scores * scale[0]
    powers = jnp.exp(scores - jnp.max(scores, axis=-1, keepdims=True))
    probs = (powers / jnp.sum(powers, axis=-1, keepdims=True)).astype(BF)
    mixed = dot(probs, rounded(2)).astype(BF)
    for n in range(copies):
        out[n, :, :HEAD] = mixed
    copy.wait()
    for m in range(columns // 256):
        at = slice(m * 256, (m + 1) * 256)
        inner = summed(slice(3 * HEAD + m * 256, 3 * HEAD + (m + 1) * 256)) + kept[at]
        activ = (inner * (0.5 + 0.5 * lax.erf(inner * math.sqrt(0.5)))).astype(BF)
        for n in range(copies):
            out[n, :, HEAD + m * 256 : HEAD + (m + 1) * 256] = activ


def middle(arrived, bias, scale):
    _, patches, _ = arrived.shape
    columns = bias.shape[0]
    return pl.pallas_call(
        middle_kernel,
        out_shape=jax.ShapeDtypeStruct((1, patches, HEAD + columns), BF),
        in_specs=[VMEM, ANY, pl.BlockSpec(memory_space=pltpu.SMEM)],
        out_specs=VMEM,
        scratch_shapes=[pltpu.VMEM((columns,), F32), pltpu.SemaphoreType.DMA],
        compiler_params=params(12),
        cost_estimate=cost(60 * patches * columns, 2 * 1024 * 1024),
        name="middle",
    )(arrived, bias, scale)


def output_kernel(part, features, *refs):
    weights, out = refs[:-1], refs[-1]
    images, half, _ = out.shape
    cols = weights[0].shape[1]
    left = features[:, part * half : (part + 1) * half].reshape(images * half, -1)
    for n, source in enumerate(weights):
        for m in range(2):
            at = slice(m * cols // 2, (m + 1) * cols // 2)
            value = dot(left, source[:, at]).astype(out.dtype)
            to = slice(n * cols + m * cols // 2, n * cols + (m + 1) * cols // 2)
            out[:, :, to] = value.reshape(images, half, cols // 2)


def output(features, weights, part, kind):
    images, patches, width = features.shape
    half, cols = patches // 2, weights[0].shape[1] * len(weights)
    return pl.pallas_call(
        functools.partial(output_kernel, part),
        out_shape=jax.ShapeDtypeStruct((images, half, cols), kind),
        in_specs=[VMEM] * (1 + len(weights)),
        out_specs=VMEM,
        compiler_params=params(16),
        cost_estimate=cost(2 * images * half * width * cols, 2 * 1024 * 1024),
        name="output_sent" if part else "output_kept",
    )(features, *weights)


def combine_kernel(n_xh, kept, received, received_p, out):
    images, half, _ = kept.shape
    n_z = half // 8
    count = 8 // n_xh
    for y in range(images):
        for z in range(n_z):
            at = slice(z * 8, (z + 1) * 8)
            for n, source in enumerate((received, received_p)):
                cols = source.shape[-1]
                to = slice(n * cols, (n + 1) * cols)
                value = kept[y, at, to] + source[y, at].astype(F32)
                for xh in range(n_xh):
                    out[(xh * n_z + z) * images + y, :, to] = value[
                        xh * count : (xh + 1) * count
                    ].astype(BF)


def combine(kept, received, received_p, n_xh):
    images, half, width = kept.shape
    count = 8 // n_xh
    return pl.pallas_call(
        functools.partial(combine_kernel, n_xh),
        out_shape=jax.ShapeDtypeStruct((images * half // count, count, width), BF),
        in_specs=[VMEM] * 3,
        out_specs=VMEM,
        compiler_params=params(8),
        cost_estimate=cost(kept.size, 4 * 1024 * 1024),
        name="combine",
    )(kept, received, received_p)


def finish_kernel(n_y, arrived, tokens, out):
    pieces, _, width = arrived.shape
    cols = width // 2
    lower = lax.axis_index("xl") == 0
    for y in range(n_y):
        total = arrived[y].astype(F32)
        for n in range(y + n_y, pieces, n_y):
            total = total + arrived[n].astype(F32)
        left, right = total[:, :cols], total[:, cols:]
        for n, value in enumerate(
            (jnp.where(lower, left, right), jnp.where(lower, right, left))
        ):
            to = slice((n * n_y + y) * cols, (n * n_y + y + 1) * cols)
            out[:, to] = (tokens[:, to].astype(F32) + value).astype(BF)


def finish(arrived, tokens, n_y):
    return pl.pallas_call(
        functools.partial(finish_kernel, n_y),
        out_shape=jax.ShapeDtypeStruct(tokens.shape, BF),
        in_specs=[VMEM] * 2,
        out_specs=VMEM,
        compiler_params=params(8),
        cost_estimate=cost(arrived.size, 2 * 1024 * 1024),
        name="finish",
    )(arrived, tokens)


def block(
    tokens, norm_gain, w_query, w_key, w_value, w_inner, bias_inner, w_attn_out, w_outer, temper
):
    n_y, n_z, n_xh = (lax.axis_size(a) for a in ("y", "z", "xh"))
    beside = partner(tokens, "xh")
    w_qkv = jnp.concatenate((w_query, w_key, w_value), axis=1)
    w_inner_p = partner(w_inner, "xl")
    w_qkv_p = partner(w_qkv, "xl")
    w_out = jnp.concatenate((w_attn_out, w_outer), axis=0)
    w_out_p = partner(w_out, "xl")
    normed, gain = norm_own(tokens, norm_gain)
    pieces = spread(normed, gain, beside, n_y, n_z)
    mine = exchange(pieces, ("z", "y"))
    theirs = partner(mine, "c")
    inner_mine = inner_part(mine, w_inner, w_inner_p, n_y)
    inner_theirs = inner_part(theirs, w_inner, w_inner_p, n_y)
    partial = heads_part(mine, theirs, w_qkv, w_qkv_p, inner_mine, inner_theirs)
    arrived = exchange(partial, "y")
    scale = temper / math.sqrt(HEAD)
    features = middle(arrived, bias_inner, scale)[0]
    features = lax.all_gather(features, "y", axis=0, tiled=False)
    sent = partner(output(features, (w_out,), 1, BF), "c")
    sent_p = partner(output(features, (w_out_p,), 1, BF), "c")
    kept = output(features, (w_out, w_out_p), 0, F32)
    pieces = combine(kept, sent, sent_p, n_xh)
    arrived = exchange(pieces, ("xh", "z", "y"))
    return finish(arrived, tokens, n_y)


def solution(mesh):
    finer = Mesh(mesh.devices.reshape(2, 4, 8, 2, 2), ALL)
    return jax.shard_map(
        block,
        mesh=finer,
        in_specs=(
            P(ALL, None),
            P(),
            P(DP, MP),
            P(DP, MP),
            P(DP, MP),
            P(DP, MP),
            P(MP),
            P(MP, DP),
            P(MP, DP),
            P(MP),
        ),
        out_specs=P(ALL, None),
        check_vma=False,
    )
```
